128 devices in a mesh: bx: 16 (over x, z_lo, core), by: 8 (over z_hi, y).
Axes of the slice: x: 4, y: 4, z: 4 (z_hi: 2, z_lo: 2; z = z_hi * 2 + z_lo), core: 2. Of those that a mesh axis runs over, the one named last changes fastest.
Arguments:
- photon_data: float32 [6, 1024, 256, 128], P(None, 'bx', 'by'), may hold values from 0 to 1, as said below
- block_counts: int32 [1024, 256], P('bx', 'by'), may hold values from 1 to 128
- gather_offsets: float32 [3, 524288], P(None, ('bx', 'by')), may hold values from 0 to 1, as said below
- gather_blocks: int32 [4, 524288], P(None, ('bx', 'by')), may hold values from 0 to 262143, as said below
- albedo: float32 [3, 524288], P(None, ('bx', 'by')), may hold values from 0.1 to 1
- gather_pixels: int32 [524288], P(('bx', 'by')), may hold values from 0 to 262143, as said below
- tile_slot: int32 [1024], replicated, may hold values from 0 to 1023, as said below
Outputs:
- film: float32 [3, 1024, 256], P(None, ('bx', 'by'))
The draws below stay inside these ranges and needn't reach their ends.
Inputs may be any that keep to these rules, and one draw needn't show every extreme that they name: `photon_data`: per point and channel in cell units: entries 0 to 2 are a position in [0, 1), entries 3 to 5 a positive power. `gather_offsets`: each coordinate lies in [0, 1). `gather_blocks`: entry 0 is the point's own cell, inside the brick of the device that holds the point; the 4 entries are the four different cells of a 2 x 2 square of cells (periodic) that contains it. `gather_pixels`: in the rows of one device, at most 96 gather points lie in tiles whose slots s share s // 8; in every draw some such owner group receives exactly 96 from every device. `tile_slot`: A permutation of 0 to 1023.
All inputs are finite; a program needn't handle non-finite values.
Results may differ from the reference program's by a relative error of at most 0.0003.
Values sent between devices are 32-bit elements; how exact they have to be, the bound alone decides.
A program may use at most 512 MiB of HBM per device.

```python
import math
import jax
import jax.numpy as jnp
from jax import lax

CX = 64
CY = 32
SLOTS = 128
LISTED = 4
G_DEV = 4096
TILE_PIX = 256
TILE_DEV = 8
OWNERS = 128
NXC = 1024
NYC = 256
NG = 524288
TILES = 1024
CAP = 96


def gather_geometry(key):
    base = jax.random.fold_in(key, 11)
    keys = jax.random.split(base, 5)
    rows = jnp.arange(NG, dtype=jnp.int32)
    device = rows // G_DEV
    bricks_y = NYC // CY
    home_x = device // bricks_y * CX + jax.random.randint(keys[0], (NG,), 0, CX)
    home_y = device % bricks_y * CY + jax.random.randint(keys[1], (NG,), 0, CY)
    step_x = 2 * jax.random.randint(keys[2], (NG,), 0, 2) - 1
    step_y = 2 * jax.random.randint(keys[3], (NG,), 0, 2) - 1
    turn = jax.random.randint(keys[4], (NG,), 0, 3)
    return (home_x, home_y, step_x, step_y, turn)


def owner_plan(key):
    base = jax.random.fold_in(key, 23)
    keys = jax.random.split(base, 5)
    perm = jax.random.permutation(keys[0], TILES).astype(jnp.int32)
    pool = OWNERS * CAP
    heavy = jax.random.randint(keys[1], (), 0, OWNERS)
    owner_of = jnp.arange(pool, dtype=jnp.int32) // CAP

    def one_device(dev_key):
        scores = jax.random.permutation(dev_key, pool).astype(jnp.int32)
        order = jnp.argsort(jnp.where(owner_of == heavy, 0, pool) + scores, stable=True)
        picked = order[:G_DEV] // CAP
        mixing = jax.random.permutation(jax.random.fold_in(dev_key, 1), G_DEV)
        return picked[mixing].astype(jnp.int32)
    dev_keys = jax.vmap(lambda d: jax.random.fold_in(keys[2], d))(jnp.arange(OWNERS))
    owner = jax.vmap(one_device)(dev_keys).reshape(NG)
    local_tile = jax.random.randint(keys[3], (NG,), 0, TILE_DEV)
    slot = owner * TILE_DEV + local_tile
    inverse = jnp.argsort(perm, stable=True).astype(jnp.int32)
    tile = inverse[slot]
    pixel = tile * TILE_PIX + jax.random.randint(keys[4], (NG,), 0, TILE_PIX)
    return (perm, pixel.astype(jnp.int32))


def draw_tile_slot(key, part):
    return owner_plan(key)[0]


def draw_gather_pixels(key, part):
    return owner_plan(key)[1]


def draw_gather_blocks(key, part):
    home_x, home_y, step_x, step_y, turn = gather_geometry(key)
    own = home_x * NYC + home_y
    beside_x = (home_x + step_x) % NXC * NYC + home_y
    beside_y = home_x * NYC + (home_y + step_y) % NYC
    beside_xy = (home_x + step_x) % NXC * NYC + (home_y + step_y) % NYC
    others = jnp.stack([beside_x, beside_y, beside_xy])
    picks = []
    for entry in range(3):
        which = (entry + turn) % 3
        picks.append(jnp.where(which == 0, others[0], jnp.where(which == 1, others[1], others[2])))
    return jnp.stack([own] + picks).astype(jnp.int32)


def draw_gather_offsets(key, part):
    home_x, home_y, step_x, step_y, turn = gather_geometry(key)
    uniforms = jax.random.uniform(jax.random.fold_in(key, 12), (3, NG), jnp.float32, 0.0, 0.999)
    off_x = jnp.where(step_x > 0, 0.5 + 0.49 * uniforms[0], 0.5 - 0.5 * uniforms[0])
    off_y = jnp.where(step_y > 0, 0.5 + 0.49 * uniforms[1], 0.5 - 0.5 * uniforms[1])
    return jnp.stack([off_x, off_y, uniforms[2]]).astype(jnp.float32)


def draw_photon_data(key, part):
    keys = jax.random.split(jax.random.fold_in(key, 31), 2)
    places = jax.random.uniform(keys[0], (3, NXC, NYC, SLOTS), jnp.float32, 0.0, 0.999)
    log_power = jax.random.uniform(keys[1], (3, NXC, NYC, SLOTS), jnp.float32, jnp.log(0.02), jnp.log(0.2))
    power = jnp.exp(log_power)
    return jnp.concatenate([places, power], axis=0).astype(jnp.float32)


def place_ends(result, rng, smallest, largest):
    longest = result.shape.index(max(result.shape))
    spots = []
    for shift in (0, 1):
        where = [jax.random.randint(jax.random.fold_in(rng, axis), (), 0, length) for axis, length in enumerate(result.shape)]
        where[longest] = (where[longest] + shift) % result.shape[longest]
        spots.append(tuple(where))
    return result.at[spots[0]].set(smallest).at[spots[1]].set(largest)


def block_scale(own_key, dims, cuts, low, largest):
    factor_of, own = 1.0, jax.random.fold_in(own_key, 6)
    for position, blocks in cuts:
        draws = jnp.exp(jax.random.uniform(jax.random.fold_in(own, position), (blocks,), jnp.float32, low / len(cuts), largest / len(cuts)))
        factor_of = factor_of * jnp.repeat(draws, dims[position] // blocks).reshape([-1 if axis == position else 1 for axis in range(len(dims))])
    return factor_of


def setup_inputs(seed: int = 0) -> dict:
    splits = jax.random.split(jax.random.key(seed), 8)
    return {
        "photon_data": draw_photon_data(jax.random.fold_in(splits[7], 71), 0),
        "block_counts": place_ends(jax.random.randint(splits[1], (NXC, NYC), 1, SLOTS + 1), jax.random.fold_in(splits[1], 1), 1, SLOTS).astype(jnp.int32),
        "gather_offsets": draw_gather_offsets(jax.random.fold_in(splits[7], 71), 0),
        "gather_blocks": draw_gather_blocks(jax.random.fold_in(splits[7], 71), 0),
        "albedo": jnp.clip(jnp.exp(math.log(1.0) - 2.3025851 * jax.random.uniform(splits[4], (3, NG), jnp.float32) ** block_scale(splits[4], (3, NG), ((1, 128),), -0.2, 0.2)), 0.1, 1.0),
        "gather_pixels": draw_gather_pixels(jax.random.fold_in(splits[7], 71), 0),
        "tile_slot": draw_tile_slot(jax.random.fold_in(splits[7], 71), 0),
    }


RADIUS_SQ = 0.25


def kernel_sum(blocks, live, shift_x, shift_y, offsets, albedo):
    delta_x = (shift_x[:, :, None] + blocks[0]) - offsets[0][:, None, None]
    delta_y = (shift_y[:, :, None] + blocks[1]) - offsets[1][:, None, None]
    delta_z = blocks[2] - offsets[2][:, None, None]
    dist_sq = delta_x * delta_x + delta_y * delta_y + delta_z * delta_z
    weight = jnp.maximum(1.0 - dist_sq / RADIUS_SQ, 0.0)
    weight = jnp.where(live, weight, 0.0)
    sums = jnp.sum(weight[None] * blocks[3:6], axis=(2, 3))
    return albedo * sums


def reference(photon_data, block_counts, gather_offsets, gather_blocks, albedo, gather_pixels, tile_slot):
    slots = photon_data.shape[3]
    table = photon_data.reshape(6, NXC * NYC, slots)
    count_table = block_counts.reshape(NXC * NYC)
    group = math.gcd(NG, 4096)
    groups = NG // group
    ids = gather_blocks.reshape(LISTED, groups, group).transpose(1, 2, 0)
    offs = gather_offsets.reshape(3, groups, group).transpose(1, 0, 2)
    albs = albedo.reshape(3, groups, group).transpose(1, 0, 2)

    def one_group(packed):
        idb, off, alb = packed
        cell_x = idb // NYC
        cell_y = idb % NYC
        shift_x = ((cell_x - cell_x[:, :1] + 1) % NXC - 1).astype(jnp.float32)
        shift_y = ((cell_y - cell_y[:, :1] + 1) % NYC - 1).astype(jnp.float32)
        flat = idb.reshape(-1)
        blocks = jnp.take(table, flat, axis=1).reshape(6, group, LISTED, slots)
        counts = jnp.take(count_table, flat).reshape(group, LISTED)
        live = jnp.arange(slots, dtype=jnp.int32)[None, None, :] < counts[:, :, None]
        return kernel_sum(blocks, live, shift_x, shift_y, off, alb)

    rad = lax.map(one_group, (ids, offs, albs))
    radiance = rad.transpose(1, 0, 2).reshape(3, NG)
    tile = gather_pixels // TILE_PIX
    slot = jnp.take(tile_slot, tile)
    target = slot * TILE_PIX + gather_pixels % TILE_PIX
    film = jnp.zeros((3, TILES * TILE_PIX), jnp.float32).at[:, target].add(radiance)
    return film.reshape(3, TILES, TILE_PIX)
```

```python
import jax
import jax.numpy as jnp
from jax import lax
from jax.experimental import pallas as pl
from jax.experimental.pallas import tpu as pltpu
from jax.sharding import PartitionSpec as P

MESH = pl.DeviceIdType.MESH
F32, BF16, I32 = jnp.float32, jnp.bfloat16, jnp.int32
CX, CY, SLOTS, G = 64, 32, 128, 4096
NXC, NYC = 1024, 256
PITCH = 2 * (CY + 2)
PAD = 8
NR = 4432
FAR = 1.0e9
OWNERS = 128
TILES = G // 128


def iota(shape, dim):
    return lax.broadcasted_iota(I32, shape, dim)


def split(x):
    high = x.astype(BF16).astype(F32)
    return high, x - high


def build_table(ph, cnt, xf, yf, table, cb):
    eye = iota((CY, CY), 0) == iota((CY, CY), 1)
    spread = jnp.where(eye[None], cnt[...][:, None, :], 0.0).reshape(CX * CY, CY)
    cb[...] = jnp.dot(spread.astype(BF16), jnp.ones((CY, SLOTS), BF16), preferred_element_type=F32)
    slot = iota((8, SLOTS), 1).astype(F32)
    sub = iota((8, SLOTS), 0).astype(F32)

    def change(c, v, x, y):
        if c == 0:
            return 2.0 * (v + x)
        if c == 1:
            return 2.0 * (v + y)
        return 2.0 * v if c == 2 else v

    def put(c, x, n, v, first, last):
        base = c * NR + PAD + x * PITCH + 2 * (1 + 8 * n)
        if not last:
            table[pl.ds(base, 8, stride=2), :] = v
        if not first:
            table[pl.ds(base - PITCH + 1, 8, stride=2), :] = v

    def one_x(x, carry):
        xs = (x + 1).astype(F32)
        for n in range(CY // 8):
            live = slot < cb[pl.ds(x * CY + 8 * n, 8), :]
            for c in range(6):
                v = change(c, ph[c, x, 8 * n : 8 * n + 8, :], xs, sub + (1.0 + 8 * n))
                if c == 0:
                    v = jnp.where(live, v, FAR)
                put(c, x + 1, n, v, False, False)
        return carry

    lax.fori_loop(0, CX, one_x, 0)
    for side, x in ((0, 0), (1, CX + 1)):
        for n in range(CY // 8):
            for c in range(6):
                v = change(c, xf[side, c, 8 * n : 8 * n + 8, :], float(x), sub + (1.0 + 8 * n))
                put(c, x, n, v, side == 0, side == 1)
    for side, y in ((0, 0), (1, CY + 1)):
        for c in range(6):
            for shift in (0, 1):
                for n in range(9):
                    rows = 8 if n < 8 else 1
                    xs = sub[:rows] + float(8 * n + shift)
                    v = change(c, yf[side, c, pl.ds(8 * n + shift, rows), :], xs, float(y))
                    base = c * NR + PAD + 8 * n * PITCH + 2 * y + shift
                    table[pl.ds(base, rows, stride=PITCH), :] = v


def sum_photons(idx, off, table, prod, sums):
    half = iota((8, SLOTS), 0) < 4

    def chunk(i, carry):
        for u in range(2):
            g0 = i * 16 + 8 * u
            for pair in range(4):
                p, q = g0 + 2 * pair, g0 + 2 * pair + 1
                rp, rq = idx[p], idx[q] - 4
                v = []
                for c in range(6):
                    a = table[pl.ds(rp + c * NR, 8), :]
                    b = table[pl.ds(rq + c * NR, 8), :]
                    if c < 3:
                        a, b = a - off[c * G + p], b - off[c * G + q]
                    v.append(jnp.where(half, a, b))
                w = jnp.maximum(1.0 - (v[0] * v[0] + v[1] * v[1] + v[2] * v[2]), 0.0)
                for c in range(3):
                    prod[c, u, 8 * pair : 8 * pair + 8, :] = w * v[3 + c]
            for c in range(3):
                s = [prod[c, u, pl.ds(k, 8, stride=4), :] for k in range(4)]
                sums[c, pl.ds(pl.multiple_of(g0, 8), 8), :] = (s[0] + s[1]) + (s[2] + s[3])
        return carry

    lax.fori_loop(0, G // 16, chunk, 0)


def pack(alb, pix, ts, sums, out, lhs, rt, carry):
    t = ts[...]
    lookup = jnp.concatenate([t >> 3, t & 7], axis=0).astype(F32).astype(BF16)
    rows = iota((128, 128), 0)
    cols = iota((128, 128), 1)
    eye = rows == cols
    before = jnp.where(rows < cols, 1.0, 0.0).astype(BF16)
    ones = jnp.ones((128, 128), BF16)
    before = jnp.concatenate([before, ones], axis=1)
    eight = iota((8, 128), 0)
    carry[...] = jnp.zeros((128, 128), F32)

    def tile(j, unused):
        at = pl.ds(pl.multiple_of(j * 128, 128), 128)
        pixel = pix[pl.ds(j, 1), :]
        image = pixel >> 8
        hot = (rows == (image & 127)).astype(F32).astype(BF16)
        found = jnp.dot(lookup, hot, preferred_element_type=F32)
        pick = eight == (image >> 7)
        owner = jnp.sum(jnp.where(pick, found[:8], 0.0), axis=0, keepdims=True)
        inner = jnp.sum(jnp.where(pick, found[8:], 0.0), axis=0, keepdims=True)
        mine = rows == owner.astype(I32)
        counts = jnp.dot(mine.astype(F32).astype(BF16), before, preferred_element_type=F32)
        rank = jnp.sum(jnp.where(mine, counts[:, :128] + carry[...], 0.0), axis=0, keepdims=True)
        carry[...] += counts[:, 128:]
        rt[:, at] = (rows == rank.astype(I32)).astype(F32).astype(BF16)
        local = inner * 256.0 + (pixel & 255).astype(F32)
        high = jnp.floor(local * (1.0 / 128.0))
        kinds = []
        for c in range(3):
            a, b = split(sums[c, at, :])
            total = jnp.dot(a.astype(BF16), ones, preferred_element_type=F32)
            total += jnp.dot(b.astype(BF16), ones, preferred_element_type=F32)
            row = jnp.sum(jnp.where(eye, total, 0.0), axis=0, keepdims=True)
            kinds.extend(split(row * alb[c, pl.ds(j, 1), :]))
        kinds.extend([high, local - 128.0 * high])
        for k, row in enumerate(kinds):
            lhs[128 * k : 128 * k + 128, at] = jnp.where(mine, row, 0.0).astype(BF16)
        return unused

    lax.fori_loop(0, TILES, tile, 0)
    for c in range(4):
        part = lax.dot_general(
            lhs[256 * c : 256 * c + 256, :], rt[...], (((1,), (1,)), ((), ())), preferred_element_type=F32
        )
        a, b = part[:128], part[128:]
        out[pl.ds(c, 128, stride=4), :] = a + b if c < 3 else 128.0 * a + b


def radiance_kernel(idx, off, ph, cnt, xf, yf, alb, pix, ts, out, table, cb, prod, sums, lhs, rt, carry):
    build_table(ph, cnt, xf, yf, table, cb)
    sum_photons(idx, off, table, prod, sums)
    pack(alb, pix, ts, sums, out, lhs, rt, carry)


def radiance_call(idx, off, ph, cnt, xf, yf, alb, pix, ts):
    smem = pl.BlockSpec(memory_space=pltpu.SMEM)
    vmem = pl.BlockSpec(memory_space=pltpu.VMEM)
    return pl.pallas_call(
        radiance_kernel,
        out_shape=jax.ShapeDtypeStruct((4 * OWNERS, 128), F32),
        in_specs=[smem] * 2 + [vmem] * 7,
        out_specs=vmem,
        scratch_shapes=[
            pltpu.VMEM((6 * NR, SLOTS), F32),
            pltpu.VMEM((CX * CY, SLOTS), F32),
            pltpu.VMEM((3, 2, 32, SLOTS), F32),
            pltpu.VMEM((3, G, SLOTS), F32),
            pltpu.VMEM((8 * 128, G), BF16),
            pltpu.VMEM((128, G), BF16),
            pltpu.VMEM((128, 128), F32),
        ],
        compiler_params=pltpu.CompilerParams(vmem_limit_bytes=60 << 20),
        name="radiance",
    )(idx, off, ph, cnt, xf, yf, alb, pix, ts)


def film_kernel(got, film, lhs, rt):
    rows = iota((128, 128), 0)
    sixteen = iota((16, 128), 0)

    def source(s, unused):
        at = pl.ds(pl.multiple_of(s * 128, 128), 128)
        pixel = got[pl.ds(4 * s + 3, 1), :].astype(I32)
        rt[:, at] = (rows == (pixel & 127)).astype(F32).astype(BF16)
        spot = sixteen == ((pixel >> 7) & 1) * 8 + (pixel >> 8)
        for c in range(3):
            for k, part in enumerate(split(got[pl.ds(4 * s + c, 1), :])):
                at_row = 16 * (2 * c + k)
                lhs[at_row : at_row + 16, at] = jnp.where(spot, part, 0.0).astype(BF16)
        return unused

    lax.fori_loop(0, OWNERS, source, 0)
    total = lax.dot_general(lhs[...], rt[...], (((1,), (1,)), ((), ())), preferred_element_type=F32)
    for c in range(3):
        both = total[32 * c : 32 * c + 16] + total[32 * c + 16 : 32 * c + 32]
        film[c, :, 0:128] = both[:8]
        film[c, :, 128:256] = both[8:]


def film_call(got):
    vmem = pl.BlockSpec(memory_space=pltpu.VMEM)
    return pl.pallas_call(
        film_kernel,
        out_shape=jax.ShapeDtypeStruct((3, 8, 256), F32),
        in_specs=[vmem],
        out_specs=vmem,
        scratch_shapes=[pltpu.VMEM((96, OWNERS * 128), BF16), pltpu.VMEM((128, OWNERS * 128), BF16)],
        compiler_params=pltpu.CompilerParams(vmem_limit_bytes=60 << 20),
        name="film",
    )(got)


def exchange_kernel(send, got, send_sem, recv_sem, own_sem):
    nx, ny = lax.axis_size("bx"), lax.axis_size("by")
    n = nx * ny
    me = lax.axis_index("bx") * ny + lax.axis_index("by")
    barrier = pltpu.get_barrier_semaphore()

    def greet(k, unused):
        peer = lax.rem(me + k, n)
        pl.semaphore_signal(barrier, inc=1, device_id=(peer // ny, lax.rem(peer, ny)), device_id_type=MESH)
        return unused

    lax.fori_loop(1, n, greet, 0)
    own = pltpu.make_async_copy(send.at[pl.ds(me, 1)], got.at[pl.ds(me, 1)], own_sem)
    own.start()
    pl.semaphore_wait(barrier, n - 1)

    def ship(k, unused):
        peer = lax.rem(me + k, n)
        pltpu.make_async_remote_copy(
            src_ref=send.at[pl.ds(peer, 1)],
            dst_ref=got.at[pl.ds(me, 1)],
            send_sem=send_sem,
            recv_sem=recv_sem,
            device_id=(peer // ny, lax.rem(peer, ny)),
            device_id_type=MESH,
        ).start()
        return unused

    lax.fori_loop(1, n, ship, 0)
    own.wait()
    for sem in (send_sem, recv_sem):
        pltpu.make_async_copy(send.at[pl.ds(0, n - 1)], got.at[pl.ds(0, n - 1)], sem).wait()


def exchange_call(blocks):
    vmem = pl.BlockSpec(memory_space=pltpu.VMEM)
    return pl.pallas_call(
        exchange_kernel,
        out_shape=jax.ShapeDtypeStruct(blocks.shape, F32),
        in_specs=[vmem],
        out_specs=vmem,
        scratch_shapes=[pltpu.SemaphoreType.DMA, pltpu.SemaphoreType.DMA, pltpu.SemaphoreType.DMA],
        compiler_params=pltpu.CompilerParams(collective_id=1, has_side_effects=True),
        name="exchange",
    )(blocks)


def ring(n):
    up = [(i, (i + 1) % n) for i in range(n)]
    return up, [(j, i) for i, j in up]


def per_device(photon_data, block_counts, gather_offsets, gather_blocks, albedo, gather_pixels, tile_slot):
    ix, iy = lax.axis_index("bx"), lax.axis_index("by")
    nx, ny = lax.axis_size("bx"), lax.axis_size("by")
    slot = iota((SLOTS,), 0)

    def masked(face, counts):
        x = jnp.where(slot < counts[..., None], face[0], FAR)
        return jnp.concatenate([x[None], face[1:]], axis=0)

    up, down = ring(nx)
    xlo = lax.ppermute(masked(photon_data[:, CX - 1], block_counts[CX - 1]), "bx", up)
    xhi = lax.ppermute(masked(photon_data[:, 0], block_counts[0]), "bx", down)
    up, down = ring(ny)

    def yface(y):
        own = masked(photon_data[:, :, y], block_counts[:, y])
        return jnp.concatenate([xlo[:, y][:, None], own, xhi[:, y][:, None]], axis=1)

    ylo = lax.ppermute(yface(CY - 1), "by", up)
    yhi = lax.ppermute(yface(0), "by", down)
    lx = (gather_blocks // NYC - ix * CX + 1) % NXC
    ly = (gather_blocks % NYC - iy * CY + 1) % NYC
    index = PAD + jnp.min(lx, axis=0) * PITCH + 2 * jnp.min(ly, axis=0)
    off = 2.0 * jnp.concatenate(
        [lx[0].astype(F32) + gather_offsets[0], ly[0].astype(F32) + gather_offsets[1], gather_offsets[2]]
    )
    blocks = radiance_call(
        index,
        off,
        photon_data,
        block_counts.astype(F32),
        jnp.stack([xlo, xhi]),
        jnp.stack([ylo, yhi]),
        albedo.reshape(3, TILES, 128),
        gather_pixels.reshape(TILES, 128),
        tile_slot.reshape(8, 128),
    )
    got = exchange_call(blocks.reshape(OWNERS, 4, 128))
    return film_call(got.reshape(4 * OWNERS, 128))


def solution(mesh):
    in_specs = (
        P(None, "bx", "by", None),
        P("bx", "by"),
        P(None, ("bx", "by")),
        P(None, ("bx", "by")),
        P(None, ("bx", "by")),
        P(("bx", "by")),
        P(),
    )
    out_specs = P(None, ("bx", "by"), None)
    return jax.shard_map(per_device, mesh=mesh, in_specs=in_specs, out_specs=out_specs, check_vma=False)
```

```python
import jax
import jax.numpy as jnp
from jax import lax
from jax.experimental import pallas as pl
from jax.experimental.pallas import tpu as pltpu
from jax.sharding import PartitionSpec as P

MESH = pl.DeviceIdType.MESH
F32, BF16, I32 = jnp.float32, jnp.bfloat16, jnp.int32
NX, NY = 16, 8
N = NX * NY
CX, CY, SLOTS, G = 64, 32, 128, 4096
NXC, NYC = 1024, 256
PITCH = 2 * (CY + 2)
PAD = 8
NR = 4456
RANKS = 96
FAR = 1.0e9
GROUPS = G // 128
FACES = ((1, 0), (-1, 0), (0, 1), (0, -1), (1, 1), (1, -1), (-1, 1), (-1, -1))


def iota(shape, dim):
    return lax.broadcasted_iota(I32, shape, dim)


def hot(mask):
    return mask.astype(F32).astype(BF16)


def split(x):
    high = x.astype(BF16).astype(F32)
    return high, x - high


def across(a, b):
    return lax.dot_general(a, b, (((1,), (1,)), ((), ())), preferred_element_type=F32)


def peer_of(flat):
    return (flat >> 3, flat & 7)


def greet_all(me):
    barrier = pltpu.get_barrier_semaphore()

    def greet(k, unused):
        pl.semaphore_signal(barrier, inc=1, device_id=peer_of((me + k) & (N - 1)), device_id_type=MESH)
        return unused

    lax.fori_loop(1, N, greet, 0)
    return barrier


def prepare(blocks, goff, ix, iy, rowv):
    cells = blocks[...]
    lx = ((cells >> 8) - ix * CX + 1) & (NXC - 1)
    ly = ((cells & (NYC - 1)) - iy * CY + 1) & (NYC - 1)
    x = jnp.minimum(jnp.min(lx, axis=0, keepdims=True), CX)
    y = jnp.minimum(jnp.min(ly, axis=0, keepdims=True), CY)
    rowv[0][...] = PAD + PITCH * x + 2 * y
    rowv[1][...] = 2.0 * (lx[0:1].astype(F32) + goff[0:1, :])
    rowv[2][...] = 2.0 * (ly[0:1].astype(F32) + goff[1:2, :])
    rowv[3][...] = 2.0 * goff[2:3, :]


def spread_counts(cnt, cb):
    eye = iota((CY, CY), 0) == iota((CY, CY), 1)
    counts = cnt[...].astype(F32)
    spread = jnp.where(eye[None], counts[:, None, :], 0.0).reshape(CX * CY, CY)
    cb[...] = jnp.dot(spread.astype(BF16), jnp.ones((CY, SLOTS), BF16), preferred_element_type=F32)


def change(c, v, x, y):
    if c == 0:
        return 2.0 * (v + x)
    if c == 1:
        return 2.0 * (v + y)
    return 2.0 * v if c == 2 else v


def build_faces(ph, cb, fx, fy, fc):
    slot = iota((8, SLOTS), 1).astype(F32)
    sub = iota((8, SLOTS), 0).astype(F32)

    def cell(c, row, rows, stride, x, y):
        at = pl.ds(row, rows, stride=stride) if rows > 1 else pl.ds(row, 1)
        v = change(c, ph[c, at, :], x, y)
        return jnp.where(slot[:rows] < cb[at, :], v, FAR) if c == 0 else v

    for side, (x, to) in enumerate(((CX - 1, 0.0), (0, CX + 1.0))):
        for c in range(6):
            for n in range(CY // 8):
                fx[side, c, 8 * n : 8 * n + 8, :] = cell(c, x * CY + 8 * n, 8, 1, to, sub + (1.0 + 8 * n))
    for side, (y, to) in enumerate(((CY - 1, 0.0), (0, CY + 1.0))):
        for c in range(6):
            for n in range(CX // 8):
                fy[side, c, 8 * n : 8 * n + 8, :] = cell(c, 8 * n * CY + y, 8, CY, sub + (1.0 + 8 * n), to)
    for k, (dx, dy) in enumerate(FACES[4:]):
        x, tx = (CX - 1, 0.0) if dx > 0 else (0, CX + 1.0)
        y, ty = (CY - 1, 0.0) if dy > 0 else (0, CY + 1.0)
        for c in range(6):
            fc[k, c : c + 1, :] = cell(c, x * CY + y, 1, 1, tx, ty)


def build_own(ph, cb, table):
    slot = iota((8, SLOTS), 1).astype(F32)
    sub = iota((8, SLOTS), 0).astype(F32)

    def one_x(x, unused):
        xs = (x + 1).astype(F32)
        for n in range(CY // 8):
            at = pl.ds(pl.multiple_of(x * CY + 8 * n, 8), 8)
            live = slot < cb[at, :]
            for c in range(6):
                v = change(c, ph[c, at, :], xs, sub + (1.0 + 8 * n))
                if c == 0:
                    v = jnp.where(live, v, FAR)
                base = c * NR + PAD + (x + 1) * PITCH + 2 * (1 + 8 * n)
                table[pl.ds(base, 8, stride=2), :] = v
                table[pl.ds(base - PITCH + 1, 8, stride=2), :] = v
        return unused

    lax.fori_loop(0, CX, one_x, 0)


def build_halo(rx, ry, rc, table):
    for c in range(6):
        for side, base in enumerate((c * NR + PAD, c * NR + PAD + CX * PITCH + 1)):
            for n in range(CY // 8):
                table[pl.ds(base + 2 + 16 * n, 8, stride=2), :] = rx[side, c, 8 * n : 8 * n + 8, :]
        for side, y in enumerate((0, CY + 1)):
            for n in range(CX // 8):
                v = ry[side, c, 8 * n : 8 * n + 8, :]
                base = c * NR + PAD + (8 * n + 1) * PITCH + 2 * y
                table[pl.ds(base, 8, stride=PITCH), :] = v
                table[pl.ds(base - PITCH + 1, 8, stride=PITCH), :] = v
        for k, (dx, dy) in enumerate(FACES[4:]):
            y = 0 if dy > 0 else CY + 1
            base = c * NR + PAD + (0 if dx > 0 else CX * PITCH + 1) + 2 * y
            table[pl.ds(base, 1), :] = rc[k, c : c + 1, :]


def rank_points(pix, ts, em, rt, lhs, carry):
    t = ts[...]
    lookup = jnp.concatenate([t >> 3, t & 7], axis=0).astype(F32).astype(BF16)
    rows, cols = iota((128, 128), 0), iota((128, 128), 1)
    before = jnp.concatenate([hot(rows < cols), jnp.ones((128, 128), BF16)], axis=1)
    eight = iota((8, 128), 0)
    carry[...] = jnp.zeros((128, 128), F32)

    def tiles(i, unused):
        for u in range(4):
            j = 4 * i + u
            at = pl.ds(pl.multiple_of(j * 128, 128), 128)
            pixel = pix[pl.ds(j, 1), :]
            image = pixel >> 8
            found = jnp.dot(lookup, hot(rows == (image & 127)), preferred_element_type=F32)
            pick = eight == (image >> 7)
            owner = jnp.sum(jnp.where(pick, found[:8], 0.0), axis=0, keepdims=True)
            inner = jnp.sum(jnp.where(pick, found[8:], 0.0), axis=0, keepdims=True)
            mine = rows == owner.astype(I32)
            chosen = hot(mine)
            em[:, at] = chosen
            counts = jnp.dot(chosen, before, preferred_element_type=F32)
            rank = jnp.sum(jnp.where(mine, counts[:, :128] + carry[...], 0.0), axis=0, keepdims=True)
            carry[...] += counts[:, 128:]
            place = hot(rows == rank.astype(I32))[:RANKS]
            rt[:, at] = place
            local = inner * 256.0 + (pixel & 255).astype(F32)
            high = jnp.floor(local * (1.0 / 128.0))
            lhs[0:RANKS, at] = place * high.astype(BF16)
            lhs[RANKS : 2 * RANKS, at] = place * (local - 128.0 * high).astype(BF16)
        return unused

    lax.fori_loop(0, GROUPS // 4, tiles, 0)


def by_owner(part):
    whole = jnp.concatenate([part, jnp.zeros((128 - RANKS, 128), F32)], axis=0)
    return whole.T


def pack_pixels(em, lhs, psend):
    part = across(lhs[0 : 2 * RANKS, :], em[...])
    psend.reshape(N, 128)[...] = by_owner(128.0 * part[:RANKS] + part[RANKS:])


def weigh_tile(j, idx, off, table, prod, sums):
    half = iota((8, SLOTS), 0) < 4
    for u in range(16):
        g0 = j * 128 + 8 * u
        for pair in range(4):
            p, q = g0 + 2 * pair, g0 + 2 * pair + 1
            rp, rq = idx[0, p], idx[0, q] - 4
            v = []
            for c in range(6):
                a = table[pl.ds(rp + c * NR, 8), :]
                b = table[pl.ds(rq + c * NR, 8), :]
                if c < 3:
                    a, b = a - off[c][0, p], b - off[c][0, q]
                v.append(jnp.where(half, a, b))
            w = jnp.maximum(1.0 - (v[0] * v[0] + v[1] * v[1] + v[2] * v[2]), 0.0)
            for c in range(3):
                prod[c, u, 8 * pair : 8 * pair + 8, :] = w * v[3 + c]
        for c in range(3):
            s = [prod[c, u, pl.ds(k, 8, stride=4), :] for k in range(4)]
            sums[c, 8 * u : 8 * u + 8, :] = (s[0] + s[1]) + (s[2] + s[3])


def place_tile(j, alb, sums, rt, lhs):
    at = pl.ds(pl.multiple_of(j * 128, 128), 128)
    ones = jnp.ones((8, 256), BF16)
    place = rt[:, at]
    for c in range(3):
        whole = sums[c]
        high = whole.astype(BF16)
        low = (whole - high.astype(F32)).astype(BF16)
        total = across(ones, jnp.concatenate([high, low], axis=1))
        for k, row in enumerate(split(total[0:1] * alb[c : c + 1, at])):
            first = RANKS * (2 * c + k)
            lhs[first : first + RANKS, at] = place * row.astype(BF16)


def radiance(idx, off, table, prod, sums, alb, rt, lhs):
    def tile(j, unused):
        place_tile(jnp.maximum(j - 1, 0), alb, sums, rt, lhs)
        weigh_tile(j, idx, off, table, prod, sums)
        return unused

    sums[...] = jnp.zeros((3, 128, SLOTS), F32)
    lax.fori_loop(0, GROUPS, tile, 0)
    place_tile(GROUPS - 1, alb, sums, rt, lhs)


def pack(em, lhs, send):
    part = across(lhs[...], em[...])
    flat = send.reshape(4 * N, 128)
    for c in range(3):
        a = part[2 * c * RANKS : (2 * c + 1) * RANKS]
        b = part[(2 * c + 1) * RANKS : (2 * c + 2) * RANKS]
        flat[pl.ds(c, 128, stride=4), :] = by_owner(a + b)


def spot_pixels(pgot, spot, rt):
    rows = iota((128, 128), 0)
    sixteen = iota((16, 128), 0)

    def sources(i, unused):
        for u in range(4):
            s = 4 * i + u
            at = pl.ds(pl.multiple_of(s * 128, 128), 128)
            pixel = pgot[s].astype(I32)
            rt[:, at] = hot(rows == (pixel & 127))
            spot[:, at] = hot(sixteen == ((pixel >> 7) & 1) * 8 + (pixel >> 8))
        return unused

    lax.fori_loop(0, N // 4, sources, 0)


def film_of(got, film, spot, lhs, rt):
    def sources(i, unused):
        for u in range(4):
            s = 4 * i + u
            at = pl.ds(pl.multiple_of(s * 128, 128), 128)
            entry = got[s]
            where = spot[:, at]
            for c in range(3):
                for k, part in enumerate(split(entry[c : c + 1, :])):
                    first = 16 * (2 * c + k)
                    lhs[first : first + 16, at] = where * part.astype(BF16)
        return unused

    lax.fori_loop(0, N // 4, sources, 0)
    total = across(lhs[...], rt[...])
    for c in range(3):
        both = total[32 * c : 32 * c + 16] + total[32 * c + 16 : 32 * c + 32]
        film[c, :, 0:128] = both[:8]
        film[c, :, 128:256] = both[8:]


def ship_all(me, send, got, own_sem, send_sem, recv_sem):
    own = pltpu.make_async_copy(send.at[pl.ds(me, 1)], got.at[pl.ds(me, 1)], own_sem)
    own.start()

    def ship(k, unused):
        peer = (me + k) & (N - 1)
        pltpu.make_async_remote_copy(
            src_ref=send.at[pl.ds(peer, 1)],
            dst_ref=got.at[pl.ds(me, 1)],
            send_sem=send_sem,
            recv_sem=recv_sem,
            device_id=peer_of(peer),
            device_id_type=MESH,
        ).start()
        return unused

    lax.fori_loop(1, N, ship, 0)
    return own


def wait_all(own, send, got, send_sem, recv_sem):
    own.wait()
    for sem in (recv_sem, send_sem):
        pltpu.make_async_copy(send.at[pl.ds(0, N - 1)], got.at[pl.ds(0, N - 1)], sem).wait()


def kernel(
    blocks, goff, photons, cnt, alb, pix, ts, film,
    ph, table, cb, idxv, oxv, oyv, ozv, idx, ox, oy, oz, prod, sums, em, rt, lhs, carry,
    fx, fy, fc, rx, ry, rc, psend, pgot, send, got, spot, flhs, frt,
    ph_sem, idx_sem, own_sem, face_send, face_recv, send_sem, recv_sem, pown_sem, psend_sem, precv_sem,
):
    ix, iy = lax.axis_index("bx"), lax.axis_index("by")
    me = ix * NY + iy
    load = pltpu.make_async_copy(photons, ph, ph_sem)
    load.start()
    barrier = greet_all(me)
    rowv, row = (idxv, oxv, oyv, ozv), (idx, ox, oy, oz)
    prepare(blocks, goff, ix, iy, rowv)
    rows = [pltpu.make_async_copy(v, r, idx_sem.at[k]) for k, (v, r) in enumerate(zip(rowv, row))]
    for copy in rows:
        copy.start()
    spread_counts(cnt, cb)
    load.wait()
    build_faces(ph, cb, fx, fy, fc)
    build_own(ph, cb, table)
    pl.semaphore_wait(barrier, N - 1)
    copies = []
    for k, (dx, dy) in enumerate(FACES):
        source, target = ((fx, rx), (fy, ry), (fc, rc))[min(k // 2, 2)]
        k2 = k % 2 if k < 4 else k - 4
        copy = pltpu.make_async_remote_copy(
            src_ref=source.at[k2],
            dst_ref=target.at[k2],
            send_sem=face_send.at[k],
            recv_sem=face_recv.at[k],
            device_id=((ix + dx) & (NX - 1), (iy + dy) & (NY - 1)),
            device_id_type=MESH,
        )
        copies.append(copy)
    for k in (2, 3, 0, 1, 4, 5, 6, 7):
        copies[k].start()
    rank_points(pix, ts, em, rt, lhs, carry)
    pack_pixels(em, lhs, psend)
    pown = ship_all(me, psend, pgot, pown_sem, psend_sem, precv_sem)
    for copy in rows:
        copy.wait()
    for copy in copies:
        copy.wait()
    build_halo(rx, ry, rc, table)
    radiance(idx, (ox, oy, oz), table, prod, sums, alb, rt, lhs)
    pack(em, lhs, send)
    own = ship_all(me, send, got, own_sem, send_sem, recv_sem)
    wait_all(pown, psend, pgot, psend_sem, precv_sem)
    spot_pixels(pgot, spot, frt)
    wait_all(own, send, got, send_sem, recv_sem)
    film_of(got, film, spot, flhs, frt)


def per_device(photon_data, block_counts, gather_offsets, gather_blocks, albedo, gather_pixels, tile_slot):
    vmem = pl.BlockSpec(memory_space=pltpu.VMEM)
    dma = pltpu.SemaphoreType.DMA
    return pl.pallas_call(
        kernel,
        out_shape=jax.ShapeDtypeStruct((3, 8, 256), F32),
        in_specs=[vmem, vmem, pl.BlockSpec(memory_space=pl.ANY), vmem, vmem, vmem, vmem],
        out_specs=vmem,
        scratch_shapes=[
            pltpu.VMEM((6, CX * CY, SLOTS), F32),
            pltpu.VMEM((6 * NR, SLOTS), F32),
            pltpu.VMEM((CX * CY, SLOTS), F32),
            pltpu.VMEM((1, G), I32),
            pltpu.VMEM((1, G), F32),
            pltpu.VMEM((1, G), F32),
            pltpu.VMEM((1, G), F32),
            pltpu.SMEM((1, G), I32),
            pltpu.SMEM((1, G), F32),
            pltpu.SMEM((1, G), F32),
            pltpu.SMEM((1, G), F32),
            pltpu.VMEM((3, 16, 32, SLOTS), F32),
            pltpu.VMEM((3, 128, SLOTS), F32),
            pltpu.VMEM((128, G), BF16),
            pltpu.VMEM((RANKS, G), BF16),
            pltpu.VMEM((6 * RANKS, G), BF16),
            pltpu.VMEM((128, 128), F32),
            pltpu.VMEM((2, 6, CY, SLOTS), F32),
            pltpu.VMEM((2, 6, CX, SLOTS), F32),
            pltpu.VMEM((4, 8, SLOTS), F32),
            pltpu.VMEM((2, 6, CY, SLOTS), F32),
            pltpu.VMEM((2, 6, CX, SLOTS), F32),
            pltpu.VMEM((4, 8, SLOTS), F32),
            pltpu.VMEM((N, 1, 128), F32),
            pltpu.VMEM((N, 1, 128), F32),
            pltpu.VMEM((N, 4, 128), F32),
            pltpu.VMEM((N, 4, 128), F32),
            pltpu.VMEM((16, N * 128), BF16),
            pltpu.VMEM((96, N * 128), BF16),
            pltpu.VMEM((128, N * 128), BF16),
            dma, dma((4,)), dma, dma((8,)), dma((8,)), dma, dma, dma, dma, dma,
        ],
        compiler_params=pltpu.CompilerParams(
            vmem_limit_bytes=67043328, collective_id=1, has_side_effects=True
        ),
        name="photon_film",
    )(
        gather_blocks,
        gather_offsets,
        photon_data.reshape(6, CX * CY, SLOTS),
        block_counts,
        albedo,
        gather_pixels.reshape(GROUPS, 128),
        tile_slot.reshape(8, 128),
    )


def solution(mesh):
    in_specs = (
        P(None, "bx", "by", None),
        P("bx", "by"),
        P(None, ("bx", "by")),
        P(None, ("bx", "by")),
        P(None, ("bx", "by")),
        P(("bx", "by")),
        P(),
    )
    out_specs = P(None, ("bx", "by"), None)
    return jax.shard_map(per_device, mesh=mesh, in_specs=in_specs, out_specs=out_specs, check_vma=False)
```

```python
import jax
import jax.numpy as jnp
from jax import lax
from jax.experimental import pallas as pl
from jax.experimental.pallas import tpu as pltpu
from jax.sharding import PartitionSpec as P

MESH = pl.DeviceIdType.MESH
F32, BF16, I32 = jnp.float32, jnp.bfloat16, jnp.int32
NX, NY = 16, 8
N = NX * NY
CX, CY, SLOTS, G = 64, 32, 128, 4096
NXC, NYC = 1024, 256
PITCH = 2 * (CY + 2)
PAD = 8
NR = 4456
RANKS = 96
BLOCK = 32
FAR = 1.0e9
GROUPS = G // 128
FACES = ((1, 0), (-1, 0), (0, 1), (0, -1), (1, 1), (1, -1), (-1, 1), (-1, -1))


def iota(shape, dim):
    return lax.broadcasted_iota(I32, shape, dim)


def hot(mask):
    return mask.astype(F32).astype(BF16)


def split(x):
    high = x.astype(BF16).astype(F32)
    return high, x - high


def across(a, b):
    return lax.dot_general(a, b, (((1,), (1,)), ((), ())), preferred_element_type=F32)


def peer_of(flat):
    return (flat >> 3, flat & 7)


def greet_all(me):
    barrier = pltpu.get_barrier_semaphore()

    def greet(k, unused):
        pl.semaphore_signal(barrier, inc=1, device_id=peer_of((me + k) & (N - 1)), device_id_type=MESH)
        return unused

    lax.fori_loop(1, N, greet, 0)
    return barrier


def prepare(blocks, goff, ix, iy, rowv):
    cells = blocks[...]
    lx = ((cells >> 8) - ix * CX + 1) & (NXC - 1)
    ly = ((cells & (NYC - 1)) - iy * CY + 1) & (NYC - 1)
    x = jnp.minimum(jnp.min(lx, axis=0, keepdims=True), CX)
    y = jnp.minimum(jnp.min(ly, axis=0, keepdims=True), CY)
    rowv[0][...] = PAD + PITCH * x + 2 * y
    rowv[1][...] = 2.0 * (lx[0:1].astype(F32) + goff[0:1, :])
    rowv[2][...] = 2.0 * (ly[0:1].astype(F32) + goff[1:2, :])
    rowv[3][...] = 2.0 * goff[2:3, :]


def spread_counts(cnt, cb):
    counts = cnt[...].astype(F32)
    for x in range(CX):
        cb[x * CY : x * CY + CY, :] = jnp.broadcast_to(counts[:, x : x + 1], (CY, SLOTS))


def change(c, v, x, y):
    if c == 0:
        return 2.0 * (v + x)
    if c == 1:
        return 2.0 * (v + y)
    return 2.0 * v if c == 2 else v


def build_faces(ph, cb, fx, fy, fc):
    slot = iota((8, SLOTS), 1).astype(F32)
    sub = iota((8, SLOTS), 0).astype(F32)

    def cell(c, row, rows, stride, x, y):
        at = pl.ds(row, rows, stride=stride) if rows > 1 else pl.ds(row, 1)
        v = change(c, ph[c, at, :], x, y)
        return jnp.where(slot[:rows] < cb[at, :], v, FAR) if c == 0 else v

    for side, (x, to) in enumerate(((CX - 1, 0.0), (0, CX + 1.0))):
        for c in range(6):
            for n in range(CY // 8):
                fx[side, c, 8 * n : 8 * n + 8, :] = cell(c, x * CY + 8 * n, 8, 1, to, sub + (1.0 + 8 * n))
    for side, (y, to) in enumerate(((CY - 1, 0.0), (0, CY + 1.0))):
        for c in range(6):
            for n in range(CX // 8):
                fy[side, c, 8 * n : 8 * n + 8, :] = cell(c, 8 * n * CY + y, 8, CY, sub + (1.0 + 8 * n), to)
    for k, (dx, dy) in enumerate(FACES[4:]):
        x, tx = (CX - 1, 0.0) if dx > 0 else (0, CX + 1.0)
        y, ty = (CY - 1, 0.0) if dy > 0 else (0, CY + 1.0)
        for c in range(6):
            fc[k, c : c + 1, :] = cell(c, x * CY + y, 1, 1, tx, ty)


def build_own(ph, cb, table):
    slot = iota((8, SLOTS), 1).astype(F32)
    sub = iota((8, SLOTS), 0).astype(F32)

    def one_x(x, unused):
        xs = (x + 1).astype(F32)
        for n in range(CY // 8):
            at = pl.ds(pl.multiple_of(x * CY + 8 * n, 8), 8)
            live = slot < cb[at, :]
            for c in range(6):
                v = change(c, ph[c, at, :], xs, sub + (1.0 + 8 * n))
                if c == 0:
                    v = jnp.where(live, v, FAR)
                base = c * NR + PAD + (x + 1) * PITCH + 2 * (1 + 8 * n)
                table[pl.ds(base, 8, stride=2), :] = v
                table[pl.ds(base - PITCH + 1, 8, stride=2), :] = v
        return unused

    lax.fori_loop(0, CX, one_x, 0)


def build_halo(rx, ry, rc, table):
    for c in range(6):
        for side, base in enumerate((c * NR + PAD, c * NR + PAD + CX * PITCH + 1)):
            for n in range(CY // 8):
                table[pl.ds(base + 2 + 16 * n, 8, stride=2), :] = rx[side, c, 8 * n : 8 * n + 8, :]
        for side, y in enumerate((0, CY + 1)):
            for n in range(CX // 8):
                v = ry[side, c, 8 * n : 8 * n + 8, :]
                base = c * NR + PAD + (8 * n + 1) * PITCH + 2 * y
                table[pl.ds(base, 8, stride=PITCH), :] = v
                table[pl.ds(base - PITCH + 1, 8, stride=PITCH), :] = v
        for k, (dx, dy) in enumerate(FACES[4:]):
            y = 0 if dy > 0 else CY + 1
            base = c * NR + PAD + (0 if dx > 0 else CX * PITCH + 1) + 2 * y
            table[pl.ds(base, 1), :] = rc[k, c : c + 1, :]


def rank_points(pix, ts, em, rt, lhs, carry):
    t = ts[...]
    lookup = jnp.concatenate([t >> 3, t & 7], axis=0).astype(F32).astype(BF16)
    rows, cols = iota((128, 128), 0), iota((128, 128), 1)
    before = jnp.concatenate([hot(rows < cols), jnp.ones((128, 128), BF16)], axis=1)
    eight = iota((8, 128), 0)
    carry[...] = jnp.zeros((128, 128), F32)

    def tiles(i, unused):
        for u in range(4):
            j = 4 * i + u
            at = pl.ds(pl.multiple_of(j * 128, 128), 128)
            pixel = pix[pl.ds(j, 1), :]
            image = pixel >> 8
            found = jnp.dot(lookup, hot(rows == (image & 127)), preferred_element_type=F32)
            pick = eight == (image >> 7)
            owner = jnp.sum(jnp.where(pick, found[:8], 0.0), axis=0, keepdims=True)
            inner = jnp.sum(jnp.where(pick, found[8:], 0.0), axis=0, keepdims=True)
            mine = rows == owner.astype(I32)
            chosen = hot(mine)
            em[:, at] = chosen
            counts = jnp.dot(chosen, before, preferred_element_type=F32)
            rank = jnp.sum(jnp.where(mine, counts[:, :128] + carry[...], 0.0), axis=0, keepdims=True)
            carry[...] += counts[:, 128:]
            place = hot(rows == rank.astype(I32))[:RANKS]
            rt[:, at] = place
            local = inner * 256.0 + (pixel & 255).astype(F32)
            high = jnp.floor(local * (1.0 / 128.0))
            lhs[0:RANKS, at] = place * high.astype(BF16)
            lhs[RANKS : 2 * RANKS, at] = place * (local - 128.0 * high).astype(BF16)
        return unused

    lax.fori_loop(0, GROUPS // 4, tiles, 0)


def by_owner(part):
    whole = jnp.concatenate([part, jnp.zeros((128 - RANKS, 128), F32)], axis=0)
    return whole.T


def pack_pixels(em, lhs, psend):
    part = across(lhs[0 : 2 * RANKS, :], em[...])
    psend.reshape(N, 128)[...] = by_owner(128.0 * part[:RANKS] + part[RANKS:])


def weigh_tile(j, idx, off, table, prod, sums):
    half = iota((8, SLOTS), 0) < 4
    for u in range(16):
        g0 = j * 128 + 8 * u
        for pair in range(4):
            p, q = g0 + 2 * pair, g0 + 2 * pair + 1
            rp, rq = idx[0, p], idx[0, q] - 4
            v = []
            for c in range(6):
                a = table[pl.ds(rp + c * NR, 8), :]
                b = table[pl.ds(rq + c * NR, 8), :]
                if c < 3:
                    a, b = a - off[c][0, p], b - off[c][0, q]
                v.append(jnp.where(half, a, b))
            w = jnp.maximum(1.0 - (v[0] * v[0] + v[1] * v[1] + v[2] * v[2]), 0.0)
            for c in range(3):
                prod[c, u, 8 * pair : 8 * pair + 8, :] = w * v[3 + c]
        for c in range(3):
            s = [prod[c, u, pl.ds(k, 8, stride=4), :] for k in range(4)]
            sums[c, 8 * u : 8 * u + 8, :] = (s[0] + s[1]) + (s[2] + s[3])


def place_tile(j, alb, sums, rt, lhs):
    at = pl.ds(pl.multiple_of(j * 128, 128), 128)
    ones = jnp.ones((8, 256), BF16)
    place = rt[:, at]
    for c in range(3):
        whole = sums[c]
        high = whole.astype(BF16)
        low = (whole - high.astype(F32)).astype(BF16)
        total = across(ones, jnp.concatenate([high, low], axis=1))
        for k, row in enumerate(split(total[0:1] * alb[c : c + 1, at])):
            first = RANKS * (2 * c + k)
            lhs[first : first + RANKS, at] = place * row.astype(BF16)


def radiance(idx, off, table, prod, sums, alb, rt, lhs):
    def tile(j, unused):
        place_tile(jnp.maximum(j - 1, 0), alb, sums, rt, lhs)
        weigh_tile(j, idx, off, table, prod, sums)
        return unused

    sums[...] = jnp.zeros((3, 128, SLOTS), F32)
    lax.fori_loop(0, GROUPS, tile, 0)
    place_tile(GROUPS - 1, alb, sums, rt, lhs)


def pack(em, lhs, send):
    part = across(lhs[...], em[...])
    flat = send.reshape(4 * N, 128)
    for c in range(3):
        a = part[2 * c * RANKS : (2 * c + 1) * RANKS]
        b = part[(2 * c + 1) * RANKS : (2 * c + 2) * RANKS]
        flat[pl.ds(c, 128, stride=4), :] = by_owner(a + b)


def spot_pixels(pgot, spot, rt):
    rows = iota((128, 128), 0)
    sixteen = iota((16, 128), 0)

    def sources(i, unused):
        for u in range(4):
            s = 4 * i + u
            at = pl.ds(pl.multiple_of(s * 128, 128), 128)
            pixel = pgot[s].astype(I32)
            rt[:, at] = hot(rows == (pixel & 127))
            spot[:, at] = hot(sixteen == ((pixel >> 7) & 1) * 8 + (pixel >> 8))
        return unused

    lax.fori_loop(0, N // 4, sources, 0)


def film_part(b, got, spot, lhs, rt, total):
    def sources(i, unused):
        for u in range(4):
            s = 4 * i + u
            at = pl.ds(pl.multiple_of(s * 128, 128), 128)
            entry = got[s]
            where = spot[:, at]
            for c in range(3):
                for k, part in enumerate(split(entry[c : c + 1, :])):
                    first = 16 * (2 * c + k)
                    lhs[first : first + 16, at] = where * part.astype(BF16)
        return unused

    lax.fori_loop(b * (BLOCK // 4), (b + 1) * (BLOCK // 4), sources, 0)
    at = pl.ds(pl.multiple_of(b * (BLOCK * 128), 128), BLOCK * 128)
    total[...] += across(lhs[:, at], rt[:, at])


def film_of(film, total):
    for c in range(3):
        both = total[32 * c : 32 * c + 16, :] + total[32 * c + 16 : 32 * c + 32, :]
        film[c, :, 0:128] = both[:8]
        film[c, :, 128:256] = both[8:]


def ship_all(me, send, got, own_sem, send_sem, recv_sem):
    own = pltpu.make_async_copy(send.at[pl.ds(me, 1)], got.at[pl.ds(me, 1)], own_sem)
    own.start()

    def ship(k, unused):
        peer = (me + k) & (N - 1)
        pltpu.make_async_remote_copy(
            src_ref=send.at[pl.ds(peer, 1)],
            dst_ref=got.at[pl.ds(me, 1)],
            send_sem=send_sem,
            recv_sem=recv_sem,
            device_id=peer_of(peer),
            device_id_type=MESH,
        ).start()
        return unused

    for first in (64, 32, 96, 0):
        lax.fori_loop(max(first, 1), first + 32, ship, 0)
    return own


def wait_all(own, send, got, send_sem, recv_sem):
    own.wait()
    for sem in (recv_sem, send_sem):
        pltpu.make_async_copy(send.at[pl.ds(0, N - 1)], got.at[pl.ds(0, N - 1)], sem).wait()


def kernel(
    blocks, goff, photons, cnt, alb, pix, ts, film,
    ph, table, cb, idxv, oxv, oyv, ozv, idx, ox, oy, oz, prod, sums, em, rt, lhs, carry,
    fx, fy, fc, rx, ry, rc, psend, pgot, send, got, spot, flhs, frt, total,
    ph_sem, idx_sem, face_send, face_recv, send_sem, recv_sem, pown_sem, psend_sem, precv_sem,
):
    ix, iy = lax.axis_index("bx"), lax.axis_index("by")
    me = ix * NY + iy
    load = pltpu.make_async_copy(photons, ph, ph_sem)
    load.start()
    barrier = greet_all(me)
    spread_counts(cnt, cb)
    load.wait()
    build_faces(ph, cb, fx, fy, fc)
    pl.semaphore_wait(barrier, N - 1)
    copies = []
    for k, (dx, dy) in enumerate(FACES):
        source, target = ((fx, rx), (fy, ry), (fc, rc))[min(k // 2, 2)]
        k2 = k % 2 if k < 4 else k - 4
        copy = pltpu.make_async_remote_copy(
            src_ref=source.at[k2],
            dst_ref=target.at[k2],
            send_sem=face_send.at[k],
            recv_sem=face_recv.at[k],
            device_id=((ix + dx) & (NX - 1), (iy + dy) & (NY - 1)),
            device_id_type=MESH,
        )
        copies.append(copy)
    for k in (2, 3, 0, 1, 4, 5, 6, 7):
        copies[k].start()
    rowv, row = (idxv, oxv, oyv, ozv), (idx, ox, oy, oz)
    prepare(blocks, goff, ix, iy, rowv)
    rows = [pltpu.make_async_copy(v, r, idx_sem.at[k]) for k, (v, r) in enumerate(zip(rowv, row))]
    for copy in rows:
        copy.start()
    rank_points(pix, ts, em, rt, lhs, carry)
    pack_pixels(em, lhs, psend)
    pown = ship_all(me, psend, pgot, pown_sem, psend_sem, precv_sem)
    build_own(ph, cb, table)
    for copy in rows:
        copy.wait()
    for copy in copies:
        copy.wait()
    build_halo(rx, ry, rc, table)
    radiance(idx, (ox, oy, oz), table, prod, sums, alb, rt, lhs)
    pack(em, lhs, send)
    quarter = me // BLOCK
    own = ship_all(me, send, got, recv_sem.at[quarter], send_sem, recv_sem.at[quarter])
    wait_all(pown, psend, pgot, psend_sem, precv_sem)
    spot_pixels(pgot, spot, frt)
    total[...] = jnp.zeros((96, 128), F32)
    for step in (0, 1, 3, 2):
        b = (quarter + step) & (N // BLOCK - 1)
        pltpu.make_async_copy(send.at[pl.ds(0, BLOCK)], got.at[pl.ds(0, BLOCK)], recv_sem.at[b]).wait()
        film_part(b, got, spot, flhs, frt, total)
    film_of(film, total)
    pltpu.make_async_copy(send.at[pl.ds(0, N - 1)], got.at[pl.ds(0, N - 1)], send_sem).wait()


def per_device(photon_data, block_counts, gather_offsets, gather_blocks, albedo, gather_pixels, tile_slot):
    vmem = pl.BlockSpec(memory_space=pltpu.VMEM)
    dma = pltpu.SemaphoreType.DMA
    return pl.pallas_call(
        kernel,
        out_shape=jax.ShapeDtypeStruct((3, 8, 256), F32),
        in_specs=[vmem, vmem, pl.BlockSpec(memory_space=pl.ANY), vmem, vmem, vmem, vmem],
        out_specs=vmem,
        scratch_shapes=[
            pltpu.VMEM((6, CX * CY, SLOTS), F32),
            pltpu.VMEM((6 * NR, SLOTS), F32),
            pltpu.VMEM((CX * CY, SLOTS), F32),
            pltpu.VMEM((1, G), I32),
            pltpu.VMEM((1, G), F32),
            pltpu.VMEM((1, G), F32),
            pltpu.VMEM((1, G), F32),
            pltpu.SMEM((1, G), I32),
            pltpu.SMEM((1, G), F32),
            pltpu.SMEM((1, G), F32),
            pltpu.SMEM((1, G), F32),
            pltpu.VMEM((3, 16, 32, SLOTS), F32),
            pltpu.VMEM((3, 128, SLOTS), F32),
            pltpu.VMEM((128, G), BF16),
            pltpu.VMEM((RANKS, G), BF16),
            pltpu.VMEM((6 * RANKS, G), BF16),
            pltpu.VMEM((128, 128), F32),
            pltpu.VMEM((2, 6, CY, SLOTS), F32),
            pltpu.VMEM((2, 6, CX, SLOTS), F32),
            pltpu.VMEM((4, 8, SLOTS), F32),
            pltpu.VMEM((2, 6, CY, SLOTS), F32),
            pltpu.VMEM((2, 6, CX, SLOTS), F32),
            pltpu.VMEM((4, 8, SLOTS), F32),
            pltpu.VMEM((N, 1, 128), F32),
            pltpu.VMEM((N, 1, 128), F32),
            pltpu.VMEM((N, 4, 128), F32),
            pltpu.VMEM((N, 4, 128), F32),
            pltpu.VMEM((16, N * 128), BF16),
            pltpu.VMEM((96, N * 128), BF16),
            pltpu.VMEM((128, N * 128), BF16),
            pltpu.VMEM((96, 128), F32),
            dma, dma((4,)), dma((8,)), dma((8,)), dma, dma((4,)), dma, dma, dma,
        ],
        compiler_params=pltpu.CompilerParams(
            vmem_limit_bytes=67043328, collective_id=1, has_side_effects=True
        ),
        name="photon_film",
    )(
        gather_blocks,
        gather_offsets,
        photon_data.reshape(6, CX * CY, SLOTS),
        block_counts.T,
        albedo,
        gather_pixels.reshape(GROUPS, 128),
        tile_slot.reshape(8, 128),
    )


def solution(mesh):
    in_specs = (
        P(None, "bx", "by", None),
        P("bx", "by"),
        P(None, ("bx", "by")),
        P(None, ("bx", "by")),
        P(None, ("bx", "by")),
        P(("bx", "by")),
        P(),
    )
    out_specs = P(None, ("bx", "by"), None)
    return jax.shard_map(per_device, mesh=mesh, in_specs=in_specs, out_specs=out_specs, check_vma=False)
```

```python
import jax
import jax.numpy as jnp
from jax import lax
from jax.experimental import pallas as pl
from jax.experimental.pallas import tpu as pltpu
from jax.sharding import PartitionSpec as P

MESH = pl.DeviceIdType.MESH
F32, BF16, I32 = jnp.float32, jnp.bfloat16, jnp.int32
NX, NY = 16, 8
N = NX * NY
CX, CY, SLOTS, G = 64, 32, 128, 4096
NXC, NYC = 1024, 256
PITCH = 2 * (CY + 2)
PAD = 8
NR = 4456
RANKS = 96
BLOCK = 32
FAR = 1.0e9
GROUPS = G // 128
FACES = ((1, 0), (-1, 0), (0, 1), (0, -1), (1, 1), (1, -1), (-1, 1), (-1, -1))


def iota(shape, dim):
    return lax.broadcasted_iota(I32, shape, dim)


def hot(mask):
    return mask.astype(F32).astype(BF16)


def split(x):
    high = x.astype(BF16).astype(F32)
    return high, x - high


def across(a, b):
    return lax.dot_general(a, b, (((1,), (1,)), ((), ())), preferred_element_type=F32)


def peer_of(flat):
    return (flat >> 3, flat & 7)


def greet_all(me):
    barrier = pltpu.get_barrier_semaphore()

    def greet(k, unused):
        pl.semaphore_signal(barrier, inc=1, device_id=peer_of((me + k) & (N - 1)), device_id_type=MESH)
        return unused

    lax.fori_loop(1, N, greet, 0)
    return barrier


def prepare(blocks, goff, ix, iy, rowv):
    cells = blocks[...]
    lx = ((cells >> 8) - ix * CX + 1) & (NXC - 1)
    ly = ((cells & (NYC - 1)) - iy * CY + 1) & (NYC - 1)
    x = jnp.minimum(jnp.min(lx, axis=0, keepdims=True), CX)
    y = jnp.minimum(jnp.min(ly, axis=0, keepdims=True), CY)
    rowv[0][...] = PAD + PITCH * x + 2 * y
    rowv[1][...] = 2.0 * (lx[0:1].astype(F32) + goff[0:1, :])
    rowv[2][...] = 2.0 * (ly[0:1].astype(F32) + goff[1:2, :])
    rowv[3][...] = 2.0 * goff[2:3, :]


def spread_counts(cnt, cb):
    counts = cnt[...].astype(F32)
    for x in range(CX):
        cb[x * CY : x * CY + CY, :] = jnp.broadcast_to(counts[:, x : x + 1], (CY, SLOTS))


def change(c, v, x, y):
    if c == 0:
        return 2.0 * (v + x)
    if c == 1:
        return 2.0 * (v + y)
    return 2.0 * v if c == 2 else v


def face_cell(ph, cb, c, row, rows, stride, x, y):
    at = pl.ds(row, rows, stride=stride) if rows > 1 else pl.ds(row, 1)
    v = change(c, ph[c, at, :], x, y)
    slot = iota((rows, SLOTS), 1).astype(F32)
    return jnp.where(slot < cb[at, :], v, FAR) if c == 0 else v


def build_faces_y(ph, cb, fy, fc):
    sub = iota((8, SLOTS), 0).astype(F32)
    for side, (y, to) in enumerate(((CY - 1, 0.0), (0, CY + 1.0))):
        for c in range(6):
            for n in range(CX // 8):
                v = face_cell(ph, cb, c, 8 * n * CY + y, 8, CY, sub + (1.0 + 8 * n), to)
                fy[side, c, 8 * n : 8 * n + 8, :] = v
    for k, (dx, dy) in enumerate(FACES[4:]):
        x, tx = (CX - 1, 0.0) if dx > 0 else (0, CX + 1.0)
        y, ty = (CY - 1, 0.0) if dy > 0 else (0, CY + 1.0)
        for c in range(6):
            fc[k, c : c + 1, :] = face_cell(ph, cb, c, x * CY + y, 1, 1, tx, ty)


def build_faces_x(ph, cb, fx):
    sub = iota((8, SLOTS), 0).astype(F32)
    for side, (x, to) in enumerate(((CX - 1, 0.0), (0, CX + 1.0))):
        for c in range(6):
            for n in range(CY // 8):
                v = face_cell(ph, cb, c, x * CY + 8 * n, 8, 1, to, sub + (1.0 + 8 * n))
                fx[side, c, 8 * n : 8 * n + 8, :] = v


def build_own(ph, cb, table):
    slot = iota((8, SLOTS), 1).astype(F32)
    sub = iota((8, SLOTS), 0).astype(F32)

    def one_x(x, unused):
        xs = (x + 1).astype(F32)
        for n in range(CY // 8):
            at = pl.ds(pl.multiple_of(x * CY + 8 * n, 8), 8)
            live = slot < cb[at, :]
            for c in range(6):
                v = change(c, ph[c, at, :], xs, sub + (1.0 + 8 * n))
                if c == 0:
                    v = jnp.where(live, v, FAR)
                base = c * NR + PAD + (x + 1) * PITCH + 2 * (1 + 8 * n)
                table[pl.ds(base, 8, stride=2), :] = v
                table[pl.ds(base - PITCH + 1, 8, stride=2), :] = v
        return unused

    lax.fori_loop(0, CX, one_x, 0)


def build_halo(rx, ry, rc, table):
    for c in range(6):
        for side, base in enumerate((c * NR + PAD, c * NR + PAD + CX * PITCH + 1)):
            for n in range(CY // 8):
                table[pl.ds(base + 2 + 16 * n, 8, stride=2), :] = rx[side, c, 8 * n : 8 * n + 8, :]
        for side, y in enumerate((0, CY + 1)):
            for n in range(CX // 8):
                v = ry[side, c, 8 * n : 8 * n + 8, :]
                base = c * NR + PAD + (8 * n + 1) * PITCH + 2 * y
                table[pl.ds(base, 8, stride=PITCH), :] = v
                table[pl.ds(base - PITCH + 1, 8, stride=PITCH), :] = v
        for k, (dx, dy) in enumerate(FACES[4:]):
            y = 0 if dy > 0 else CY + 1
            base = c * NR + PAD + (0 if dx > 0 else CX * PITCH + 1) + 2 * y
            table[pl.ds(base, 1), :] = rc[k, c : c + 1, :]


def rank_points(pix, ts, em, rt, lhs, carry):
    t = ts[...]
    lookup = jnp.concatenate([t >> 3, t & 7], axis=0).astype(F32).astype(BF16)
    rows, cols = iota((128, 128), 0), iota((128, 128), 1)
    before = jnp.concatenate([hot(rows < cols), jnp.ones((128, 128), BF16)], axis=1)
    eight = iota((8, 128), 0)
    carry[...] = jnp.zeros((128, 128), F32)

    def tiles(i, unused):
        for u in range(4):
            j = 4 * i + u
            at = pl.ds(pl.multiple_of(j * 128, 128), 128)
            pixel = pix[pl.ds(j, 1), :]
            image = pixel >> 8
            found = jnp.dot(lookup, hot(rows == (image & 127)), preferred_element_type=F32)
            pick = eight == (image >> 7)
            owner = jnp.sum(jnp.where(pick, found[:8], 0.0), axis=0, keepdims=True)
            inner = jnp.sum(jnp.where(pick, found[8:], 0.0), axis=0, keepdims=True)
            mine = rows == owner.astype(I32)
            chosen = hot(mine)
            em[:, at] = chosen
            counts = jnp.dot(chosen, before, preferred_element_type=F32)
            rank = jnp.sum(jnp.where(mine, counts[:, :128] + carry[...], 0.0), axis=0, keepdims=True)
            carry[...] += counts[:, 128:]
            place = hot(rows == rank.astype(I32))[:RANKS]
            rt[:, at] = place
            local = inner * 256.0 + (pixel & 255).astype(F32)
            high = jnp.floor(local * (1.0 / 128.0))
            lhs[0:RANKS, at] = place * high.astype(BF16)
            lhs[RANKS : 2 * RANKS, at] = place * (local - 128.0 * high).astype(BF16)
        return unused

    lax.fori_loop(0, GROUPS // 4, tiles, 0)


def by_owner(part):
    whole = jnp.concatenate([part, jnp.zeros((128 - RANKS, 128), F32)], axis=0)
    return whole.T


def pack_pixels(em, lhs, psend):
    part = across(lhs[0 : 2 * RANKS, :], em[...])
    psend.reshape(N, 128)[...] = by_owner(128.0 * part[:RANKS] + part[RANKS:])


def weigh_tile(j, idx, off, table, prod, sums):
    half = iota((8, SLOTS), 0) < 4
    for u in range(16):
        g0 = j * 128 + 8 * u
        for pair in range(4):
            p, q = g0 + 2 * pair, g0 + 2 * pair + 1
            rp, rq = idx[0, p], idx[0, q] - 4
            v = []
            for c in range(6):
                a = table[pl.ds(rp + c * NR, 8), :]
                b = table[pl.ds(rq + c * NR, 8), :]
                if c < 3:
                    a, b = a - off[c][0, p], b - off[c][0, q]
                v.append(jnp.where(half, a, b))
            w = jnp.maximum(1.0 - (v[0] * v[0] + v[1] * v[1] + v[2] * v[2]), 0.0)
            for c in range(3):
                prod[c, u, 8 * pair : 8 * pair + 8, :] = w * v[3 + c]
        for c in range(3):
            s = [prod[c, u, pl.ds(k, 8, stride=4), :] for k in range(4)]
            sums[c, 8 * u : 8 * u + 8, :] = (s[0] + s[1]) + (s[2] + s[3])


def place_tile(j, alb, sums, rt, lhs):
    at = pl.ds(pl.multiple_of(j * 128, 128), 128)
    ones = jnp.ones((8, 256), BF16)
    place = rt[:, at]
    for c in range(3):
        whole = sums[c]
        high = whole.astype(BF16)
        low = (whole - high.astype(F32)).astype(BF16)
        total = across(ones, jnp.concatenate([high, low], axis=1))
        for k, row in enumerate(split(total[0:1] * alb[c : c + 1, at])):
            first = RANKS * (2 * c + k)
            lhs[first : first + RANKS, at] = place * row.astype(BF16)


def radiance(idx, off, table, prod, sums, alb, rt, lhs):
    def tiles(i, unused):
        place_tile(jnp.maximum(2 * i - 1, 0), alb, sums.at[1], rt, lhs)
        weigh_tile(2 * i, idx, off, table, prod, sums.at[0])
        place_tile(2 * i, alb, sums.at[0], rt, lhs)
        weigh_tile(2 * i + 1, idx, off, table, prod, sums.at[1])
        return unused

    sums[...] = jnp.zeros((2, 3, 128, SLOTS), F32)
    lax.fori_loop(0, GROUPS // 2, tiles, 0)
    place_tile(GROUPS - 1, alb, sums.at[1], rt, lhs)


def pack(em, lhs, send):
    part = across(lhs[...], em[...])
    flat = send.reshape(3 * N, 128)
    for c in range(3):
        a = part[2 * c * RANKS : (2 * c + 1) * RANKS]
        b = part[(2 * c + 1) * RANKS : (2 * c + 2) * RANKS]
        flat[pl.ds(c, 128, stride=3), :] = by_owner(a + b)


def spot_pixels(pgot, spot, rt):
    rows = iota((128, 128), 0)
    sixteen = iota((16, 128), 0)

    def sources(i, unused):
        for u in range(4):
            s = 4 * i + u
            at = pl.ds(pl.multiple_of(s * 128, 128), 128)
            pixel = pgot[s].astype(I32)
            rt[:, at] = hot(rows == (pixel & 127))
            spot[:, at] = hot(sixteen == ((pixel >> 7) & 1) * 8 + (pixel >> 8))
        return unused

    lax.fori_loop(0, N // 4, sources, 0)


def film_part(b, got, spot, lhs, rt, total):
    def sources(i, unused):
        for u in range(4):
            s = 4 * i + u
            at = pl.ds(pl.multiple_of(s * 128, 128), 128)
            where = spot[:, at]
            for c in range(3):
                for k, part in enumerate(split(got[3 * s + c])):
                    first = 16 * (2 * c + k)
                    lhs[first : first + 16, at] = where * part.astype(BF16)
        return unused

    lax.fori_loop(b * (BLOCK // 4), (b + 1) * (BLOCK // 4), sources, 0)
    at = pl.ds(pl.multiple_of(b * (BLOCK * 128), 128), BLOCK * 128)
    total[...] += across(lhs[:, at], rt[:, at])


def film_of(film, total):
    for c in range(3):
        both = total[32 * c : 32 * c + 16, :] + total[32 * c + 16 : 32 * c + 32, :]
        film[c, :, 0:128] = both[:8]
        film[c, :, 128:256] = both[8:]


def ship_all(me, rows, send, got, own_sem, send_sem, recv_sem):
    here = pl.ds(me * rows, rows)
    own = pltpu.make_async_copy(send.at[here], got.at[here], own_sem)
    own.start()

    def ship(k, unused):
        peer = (me + k) & (N - 1)
        pltpu.make_async_remote_copy(
            src_ref=send.at[pl.ds(peer * rows, rows)],
            dst_ref=got.at[here],
            send_sem=send_sem,
            recv_sem=recv_sem,
            device_id=peer_of(peer),
            device_id_type=MESH,
        ).start()
        return unused

    for first in (64, 32, 96, 0):
        lax.fori_loop(max(first, 1), first + 32, ship, 0)
    return own


def wait_all(own, send, got, send_sem, recv_sem):
    own.wait()
    for sem in (recv_sem, send_sem):
        pltpu.make_async_copy(send.at[pl.ds(0, N - 1)], got.at[pl.ds(0, N - 1)], sem).wait()


def kernel(
    blocks, goff, photons, cnt, alb, pix, ts, film,
    ph4, table, cb, idxv, oxv, oyv, ozv, idx, ox, oy, oz, prod, sums, em, rt, lhs, carry,
    fx, fy, fc, rx, ry, rc, psend, pgot, send, got, spot, flhs, frt, total,
    ph_sem, idx_sem, face_send, face_recv, send_sem, recv_sem, pown_sem, psend_sem, precv_sem,
):
    ix, iy = lax.axis_index("bx"), lax.axis_index("by")
    me = ix * NY + iy
    loads = []
    for k, (first, last) in enumerate(((0, 8), (CY - 8, CY), (8, CY - 8))):
        part = (slice(None), slice(None), pl.ds(first, last - first))
        loads.append(pltpu.make_async_copy(photons.at[part], ph4.at[part], ph_sem.at[k]))
        loads[k].start()
    ph = ph4.reshape(6, CX * CY, SLOTS)
    barrier = greet_all(me)
    spread_counts(cnt, cb)
    loads[0].wait()
    loads[1].wait()
    build_faces_y(ph, cb, fy, fc)
    pl.semaphore_wait(barrier, N - 1)
    copies = []
    for k, (dx, dy) in enumerate(FACES):
        source, target = ((fx, rx), (fy, ry), (fc, rc))[min(k // 2, 2)]
        k2 = k % 2 if k < 4 else k - 4
        copy = pltpu.make_async_remote_copy(
            src_ref=source.at[k2],
            dst_ref=target.at[k2],
            send_sem=face_send.at[k],
            recv_sem=face_recv.at[k],
            device_id=((ix + dx) & (NX - 1), (iy + dy) & (NY - 1)),
            device_id_type=MESH,
        )
        copies.append(copy)
    for k in (2, 3, 4, 5, 6, 7):
        copies[k].start()
    loads[2].wait()
    build_faces_x(ph, cb, fx)
    for k in (0, 1):
        copies[k].start()
    rowv, row = (idxv, oxv, oyv, ozv), (idx, ox, oy, oz)
    prepare(blocks, goff, ix, iy, rowv)
    rows = [pltpu.make_async_copy(v, r, idx_sem.at[k]) for k, (v, r) in enumerate(zip(rowv, row))]
    for copy in rows:
        copy.start()
    rank_points(pix, ts, em, rt, lhs, carry)
    pack_pixels(em, lhs, psend)
    pown = ship_all(me, 1, psend, pgot, pown_sem, psend_sem, precv_sem)
    build_own(ph, cb, table)
    for copy in rows:
        copy.wait()
    for copy in copies:
        copy.wait()
    build_halo(rx, ry, rc, table)
    radiance(idx, (ox, oy, oz), table, prod, sums, alb, rt, lhs)
    pack(em, lhs, send)
    quarter = me // BLOCK
    own = ship_all(me, 3, send, got, recv_sem.at[quarter], send_sem, recv_sem.at[quarter])
    wait_all(pown, psend, pgot, psend_sem, precv_sem)
    spot_pixels(pgot, spot, frt)
    total[...] = jnp.zeros((96, 128), F32)
    for step in (0, 1, 3, 2):
        b = (quarter + step) & (N // BLOCK - 1)
        quarter_rows = pl.ds(0, 3 * BLOCK)
        pltpu.make_async_copy(send.at[quarter_rows], got.at[quarter_rows], recv_sem.at[b]).wait()
        film_part(b, got, spot, flhs, frt, total)
    film_of(film, total)
    sent = pl.ds(0, 3 * (N - 1))
    pltpu.make_async_copy(send.at[sent], got.at[sent], send_sem).wait()


def per_device(photon_data, block_counts, gather_offsets, gather_blocks, albedo, gather_pixels, tile_slot):
    vmem = pl.BlockSpec(memory_space=pltpu.VMEM)
    dma = pltpu.SemaphoreType.DMA
    return pl.pallas_call(
        kernel,
        out_shape=jax.ShapeDtypeStruct((3, 8, 256), F32),
        in_specs=[vmem, vmem, pl.BlockSpec(memory_space=pl.ANY), vmem, vmem, vmem, vmem],
        out_specs=vmem,
        scratch_shapes=[
            pltpu.VMEM((6, CX, CY, SLOTS), F32),
            pltpu.VMEM((6 * NR, SLOTS), F32),
            pltpu.VMEM((CX * CY, SLOTS), F32),
            pltpu.VMEM((1, G), I32),
            pltpu.VMEM((1, G), F32),
            pltpu.VMEM((1, G), F32),
            pltpu.VMEM((1, G), F32),
            pltpu.SMEM((1, G), I32),
            pltpu.SMEM((1, G), F32),
            pltpu.SMEM((1, G), F32),
            pltpu.SMEM((1, G), F32),
            pltpu.VMEM((3, 16, 32, SLOTS), F32),
            pltpu.VMEM((2, 3, 128, SLOTS), F32),
            pltpu.VMEM((128, G), BF16),
            pltpu.VMEM((RANKS, G), BF16),
            pltpu.VMEM((6 * RANKS, G), BF16),
            pltpu.VMEM((128, 128), F32),
            pltpu.VMEM((2, 6, CY, SLOTS), F32),
            pltpu.VMEM((2, 6, CX, SLOTS), F32),
            pltpu.VMEM((4, 8, SLOTS), F32),
            pltpu.VMEM((2, 6, CY, SLOTS), F32),
            pltpu.VMEM((2, 6, CX, SLOTS), F32),
            pltpu.VMEM((4, 8, SLOTS), F32),
            pltpu.VMEM((N, 1, 128), F32),
            pltpu.VMEM((N, 1, 128), F32),
            pltpu.VMEM((3 * N, 1, 128), F32),
            pltpu.VMEM((3 * N, 1, 128), F32),
            pltpu.VMEM((16, N * 128), BF16),
            pltpu.VMEM((96, N * 128), BF16),
            pltpu.VMEM((128, N * 128), BF16),
            pltpu.VMEM((96, 128), F32),
            dma((3,)), dma((4,)), dma((8,)), dma((8,)), dma, dma((4,)), dma, dma, dma,
        ],
        compiler_params=pltpu.CompilerParams(
            vmem_limit_bytes=67043328, collective_id=1, has_side_effects=True
        ),
        name="photon_film",
    )(
        gather_blocks,
        gather_offsets,
        photon_data,
        block_counts.T,
        albedo,
        gather_pixels.reshape(GROUPS, 128),
        tile_slot.reshape(8, 128),
    )


def solution(mesh):
    in_specs = (
        P(None, "bx", "by", None),
        P("bx", "by"),
        P(None, ("bx", "by")),
        P(None, ("bx", "by")),
        P(None, ("bx", "by")),
        P(("bx", "by")),
        P(),
    )
    out_specs = P(None, ("bx", "by"), None)
    return jax.shard_map(per_device, mesh=mesh, in_specs=in_specs, out_specs=out_specs, check_vma=False)
```

```python
import jax
import jax.numpy as jnp
from jax import lax
from jax.experimental import pallas as pl
from jax.experimental.pallas import tpu as pltpu
from jax.sharding import PartitionSpec as P

MESH = pl.DeviceIdType.MESH
F32, BF16, I32 = jnp.float32, jnp.bfloat16, jnp.int32
NX, NY = 16, 8
N = NX * NY
CX, CY, SLOTS, G = 64, 32, 128, 4096
NXC, NYC = 1024, 256
PITCH = 2 * (CY + 2)
PAD = 8
NR = 4456
RANKS = 96
BLOCK = 32
FAR = 1.0e9
GROUPS = G // 128
FACES = ((1, 0), (-1, 0), (0, 1), (0, -1), (1, 1), (1, -1), (-1, 1), (-1, -1))


def iota(shape, dim):
    return lax.broadcasted_iota(I32, shape, dim)


def hot(mask):
    return mask.astype(F32).astype(BF16)


def split(x):
    high = x.astype(BF16).astype(F32)
    return high, x - high


def across(a, b):
    return lax.dot_general(a, b, (((1,), (1,)), ((), ())), preferred_element_type=F32)


def peer_of(flat):
    return (flat >> 3, flat & 7)


def greet_all(me):
    barrier = pltpu.get_barrier_semaphore()

    def greet(k, unused):
        pl.semaphore_signal(barrier, inc=1, device_id=peer_of((me + k) & (N - 1)), device_id_type=MESH)
        return unused

    lax.fori_loop(1, N, greet, 0)
    return barrier


def prepare(blocks, goff, ix, iy, rowv):
    cells = blocks[...]
    lx = ((cells >> 8) - ix * CX + 1) & (NXC - 1)
    ly = ((cells & (NYC - 1)) - iy * CY + 1) & (NYC - 1)
    x = jnp.minimum(jnp.min(lx, axis=0, keepdims=True), CX)
    y = jnp.minimum(jnp.min(ly, axis=0, keepdims=True), CY)
    rowv[0][...] = PAD + PITCH * x + 2 * y
    rowv[1][...] = 2.0 * (lx[0:1].astype(F32) + goff[0:1, :])
    rowv[2][...] = 2.0 * (ly[0:1].astype(F32) + goff[1:2, :])
    rowv[3][...] = 2.0 * goff[2:3, :]


def spread_counts(cnt, cb):
    counts = cnt[...].astype(F32)
    for x in range(CX):
        cb[x * CY : x * CY + CY, :] = jnp.broadcast_to(counts[:, x : x + 1], (CY, SLOTS))


def change(c, v, x, y):
    if c == 0:
        return 2.0 * (v + x)
    if c == 1:
        return 2.0 * (v + y)
    return 2.0 * v if c == 2 else v


def face_cell(ph, cb, c, row, rows, stride, x, y):
    at = pl.ds(row, rows, stride=stride) if rows > 1 else pl.ds(row, 1)
    v = change(c, ph[c, at, :], x, y)
    slot = iota((rows, SLOTS), 1).astype(F32)
    return jnp.where(slot < cb[at, :], v, FAR) if c == 0 else v


def build_faces_y(ph, cb, fy, fc):
    sub = iota((8, SLOTS), 0).astype(F32)
    for side, (y, to) in enumerate(((CY - 1, 0.0), (0, CY + 1.0))):
        for c in range(6):
            for n in range(CX // 8):
                v = face_cell(ph, cb, c, 8 * n * CY + y, 8, CY, sub + (1.0 + 8 * n), to)
                fy[side, c, 8 * n : 8 * n + 8, :] = v
    for k, (dx, dy) in enumerate(FACES[4:]):
        x, tx = (CX - 1, 0.0) if dx > 0 else (0, CX + 1.0)
        y, ty = (CY - 1, 0.0) if dy > 0 else (0, CY + 1.0)
        for c in range(6):
            fc[k, c : c + 1, :] = face_cell(ph, cb, c, x * CY + y, 1, 1, tx, ty)


def build_faces_x(ph, cb, fx):
    sub = iota((8, SLOTS), 0).astype(F32)
    for side, (x, to) in enumerate(((CX - 1, 0.0), (0, CX + 1.0))):
        for c in range(6):
            for n in range(CY // 8):
                v = face_cell(ph, cb, c, x * CY + 8 * n, 8, 1, to, sub + (1.0 + 8 * n))
                fx[side, c, 8 * n : 8 * n + 8, :] = v


def build_own(ph, cb, table):
    slot = iota((8, SLOTS), 1).astype(F32)
    sub = iota((8, SLOTS), 0).astype(F32)

    def one_x(x, unused):
        xs = (x + 1).astype(F32)
        for n in range(CY // 8):
            at = pl.ds(pl.multiple_of(x * CY + 8 * n, 8), 8)
            live = slot < cb[at, :]
            for c in range(6):
                v = change(c, ph[c, at, :], xs, sub + (1.0 + 8 * n))
                if c == 0:
                    v = jnp.where(live, v, FAR)
                base = c * NR + PAD + (x + 1) * PITCH + 2 * (1 + 8 * n)
                table[pl.ds(base, 8, stride=2), :] = v
                table[pl.ds(base - PITCH + 1, 8, stride=2), :] = v
        return unused

    lax.fori_loop(0, CX, one_x, 0)


def build_halo(rx, ry, rc, table):
    for c in range(6):
        for side, base in enumerate((c * NR + PAD, c * NR + PAD + CX * PITCH + 1)):
            for n in range(CY // 8):
                table[pl.ds(base + 2 + 16 * n, 8, stride=2), :] = rx[side, c, 8 * n : 8 * n + 8, :]
        for side, y in enumerate((0, CY + 1)):
            for n in range(CX // 8):
                v = ry[side, c, 8 * n : 8 * n + 8, :]
                base = c * NR + PAD + (8 * n + 1) * PITCH + 2 * y
                table[pl.ds(base, 8, stride=PITCH), :] = v
                table[pl.ds(base - PITCH + 1, 8, stride=PITCH), :] = v
        for k, (dx, dy) in enumerate(FACES[4:]):
            y = 0 if dy > 0 else CY + 1
            base = c * NR + PAD + (0 if dx > 0 else CX * PITCH + 1) + 2 * y
            table[pl.ds(base, 1), :] = rc[k, c : c + 1, :]


def rank_points(pix, ts, em, rt, lhs, carry):
    t = ts[...]
    lookup = jnp.concatenate([t >> 3, t & 7], axis=0).astype(F32).astype(BF16)
    rows, cols = iota((128, 128), 0), iota((128, 128), 1)
    before = jnp.concatenate([hot(rows < cols), jnp.ones((128, 128), BF16)], axis=1)
    eight = iota((8, 128), 0)
    carry[...] = jnp.zeros((128, 128), F32)

    def tiles(i, unused):
        for u in range(4):
            j = 4 * i + u
            at = pl.ds(pl.multiple_of(j * 128, 128), 128)
            pixel = pix[pl.ds(j, 1), :]
            image = pixel >> 8
            found = jnp.dot(lookup, hot(rows == (image & 127)), preferred_element_type=F32)
            pick = eight == (image >> 7)
            owner = jnp.sum(jnp.where(pick, found[:8], 0.0), axis=0, keepdims=True)
            inner = jnp.sum(jnp.where(pick, found[8:], 0.0), axis=0, keepdims=True)
            mine = rows == owner.astype(I32)
            chosen = hot(mine)
            em[:, at] = chosen
            counts = jnp.dot(chosen, before, preferred_element_type=F32)
            rank = jnp.sum(jnp.where(mine, counts[:, :128] + carry[...], 0.0), axis=0, keepdims=True)
            carry[...] += counts[:, 128:]
            place = hot(rows == rank.astype(I32))[:RANKS]
            rt[:, at] = place
            local = inner * 256.0 + (pixel & 255).astype(F32)
            high = jnp.floor(local * (1.0 / 128.0))
            lhs[0:RANKS, at] = place * high.astype(BF16)
            lhs[RANKS : 2 * RANKS, at] = place * (local - 128.0 * high).astype(BF16)
        return unused

    lax.fori_loop(0, GROUPS // 4, tiles, 0)


def by_owner(part):
    whole = jnp.concatenate([part, jnp.zeros((128 - RANKS, 128), F32)], axis=0)
    return whole.T


def pack_pixels(em, lhs, psend):
    part = across(lhs[0 : 2 * RANKS, :], em[...])
    psend.reshape(N, 128)[...] = by_owner(128.0 * part[:RANKS] + part[RANKS:])


def weigh_tile(j, idx, off, table, prod, sums, between):
    half = iota((8, SLOTS), 0) < 4
    for u in range(16):
        if u in (2, 6, 10):
            between(u // 4)
        g0 = j * 128 + 8 * u
        for pair in range(4):
            p, q = g0 + 2 * pair, g0 + 2 * pair + 1
            rp, rq = idx[0, p], idx[0, q] - 4
            v = []
            for c in range(6):
                a = table[pl.ds(rp + c * NR, 8), :]
                b = table[pl.ds(rq + c * NR, 8), :]
                if c < 3:
                    a, b = a - off[c][0, p], b - off[c][0, q]
                v.append(jnp.where(half, a, b))
            w = jnp.maximum(1.0 - (v[0] * v[0] + v[1] * v[1] + v[2] * v[2]), 0.0)
            for c in range(3):
                prod[c, u, 8 * pair : 8 * pair + 8, :] = w * v[3 + c]
        for c in range(3):
            s = [prod[c, u, pl.ds(k, 8, stride=4), :] for k in range(4)]
            sums[c, 8 * u : 8 * u + 8, :] = (s[0] + s[1]) + (s[2] + s[3])


def place_tile(j, alb, sums, rt, lhs, channels=(0, 1, 2)):
    at = pl.ds(pl.multiple_of(j * 128, 128), 128)
    ones = jnp.ones((8, 256), BF16)
    place = rt[:, at]
    for c in channels:
        whole = sums[c]
        high = whole.astype(BF16)
        low = (whole - high.astype(F32)).astype(BF16)
        total = across(ones, jnp.concatenate([high, low], axis=1))
        for k, row in enumerate(split(total[0:1] * alb[c : c + 1, at])):
            first = RANKS * (2 * c + k)
            lhs[first : first + RANKS, at] = place * row.astype(BF16)


def radiance(idx, off, table, prod, sums, alb, rt, lhs):
    def tiles(i, unused):
        for k in range(2):
            j = 2 * i + k

            def between(c):
                place_tile(jnp.maximum(j - 1, 0), alb, sums.at[1 - k], rt, lhs, (c,))

            weigh_tile(j, idx, off, table, prod, sums.at[k], between)
        return unused

    sums[...] = jnp.zeros((2, 3, 128, SLOTS), F32)
    lax.fori_loop(0, GROUPS // 2, tiles, 0)
    place_tile(GROUPS - 1, alb, sums.at[1], rt, lhs)


def pack(em, lhs, send):
    part = across(lhs[...], em[...])
    flat = send.reshape(3 * N, 128)
    for c in range(3):
        a = part[2 * c * RANKS : (2 * c + 1) * RANKS]
        b = part[(2 * c + 1) * RANKS : (2 * c + 2) * RANKS]
        flat[pl.ds(c, 128, stride=3), :] = by_owner(a + b)


def spot_pixels(pgot, spot, rt):
    rows = iota((128, 128), 0)
    sixteen = iota((16, 128), 0)

    def sources(i, unused):
        for u in range(4):
            s = 4 * i + u
            at = pl.ds(pl.multiple_of(s * 128, 128), 128)
            pixel = pgot[s].astype(I32)
            rt[:, at] = hot(rows == (pixel & 127))
            spot[:, at] = hot(sixteen == ((pixel >> 7) & 1) * 8 + (pixel >> 8))
        return unused

    lax.fori_loop(0, N // 4, sources, 0)


def film_part(b, got, spot, lhs, rt, total):
    def sources(i, unused):
        for u in range(4):
            s = 4 * i + u
            at = pl.ds(pl.multiple_of(s * 128, 128), 128)
            where = spot[:, at]
            for c in range(3):
                for k, part in enumerate(split(got[3 * s + c])):
                    first = 16 * (2 * c + k)
                    lhs[first : first + 16, at] = where * part.astype(BF16)
        return unused

    lax.fori_loop(b * (BLOCK // 4), (b + 1) * (BLOCK // 4), sources, 0)
    at = pl.ds(pl.multiple_of(b * (BLOCK * 128), 128), BLOCK * 128)
    total[...] += across(lhs[:, at], rt[:, at])


def film_of(film, total):
    for c in range(3):
        both = total[32 * c : 32 * c + 16, :] + total[32 * c + 16 : 32 * c + 32, :]
        film[c, :, 0:128] = both[:8]
        film[c, :, 128:256] = both[8:]


def ship_all(me, rows, send, got, own_sem, send_sem, recv_sem):
    here = pl.ds(me * rows, rows)
    own = pltpu.make_async_copy(send.at[here], got.at[here], own_sem)
    own.start()

    def ship(k, unused):
        peer = (me + k) & (N - 1)
        pltpu.make_async_remote_copy(
            src_ref=send.at[pl.ds(peer * rows, rows)],
            dst_ref=got.at[here],
            send_sem=send_sem,
            recv_sem=recv_sem,
            device_id=peer_of(peer),
            device_id_type=MESH,
        ).start()
        return unused

    for first in (64, 32, 96, 0):
        lax.fori_loop(max(first, 1), first + 32, ship, 0)
    return own


def wait_all(own, send, got, send_sem, recv_sem):
    own.wait()
    for sem in (recv_sem, send_sem):
        pltpu.make_async_copy(send.at[pl.ds(0, N - 1)], got.at[pl.ds(0, N - 1)], sem).wait()


def kernel(
    blocks, goff, photons, cnt, alb, pix, ts, film,
    ph4, table, cb, idxv, oxv, oyv, ozv, idx, ox, oy, oz, prod, sums, em, rt, lhs, carry,
    fx, fy, fc, rx, ry, rc, psend, pgot, send, got, spot, flhs, frt, total,
    ph_sem, idx_sem, face_send, face_recv, send_sem, recv_sem, pown_sem, psend_sem, precv_sem,
):
    ix, iy = lax.axis_index("bx"), lax.axis_index("by")
    me = ix * NY + iy
    loads = []
    for k, (first, last) in enumerate(((0, 8), (CY - 8, CY), (8, CY - 8))):
        part = (slice(None), slice(None), pl.ds(first, last - first))
        loads.append(pltpu.make_async_copy(photons.at[part], ph4.at[part], ph_sem.at[k]))
        loads[k].start()
    ph = ph4.reshape(6, CX * CY, SLOTS)
    barrier = greet_all(me)
    spread_counts(cnt, cb)
    loads[0].wait()
    loads[1].wait()
    build_faces_y(ph, cb, fy, fc)
    pl.semaphore_wait(barrier, N - 1)
    copies = []
    for k, (dx, dy) in enumerate(FACES):
        source, target = ((fx, rx), (fy, ry), (fc, rc))[min(k // 2, 2)]
        k2 = k % 2 if k < 4 else k - 4
        copy = pltpu.make_async_remote_copy(
            src_ref=source.at[k2],
            dst_ref=target.at[k2],
            send_sem=face_send.at[k],
            recv_sem=face_recv.at[k],
            device_id=((ix + dx) & (NX - 1), (iy + dy) & (NY - 1)),
            device_id_type=MESH,
        )
        copies.append(copy)
    for k in (2, 3, 4, 5, 6, 7):
        copies[k].start()
    loads[2].wait()
    build_faces_x(ph, cb, fx)
    for k in (0, 1):
        copies[k].start()
    rowv, row = (idxv, oxv, oyv, ozv), (idx, ox, oy, oz)
    prepare(blocks, goff, ix, iy, rowv)
    rows = [pltpu.make_async_copy(v, r, idx_sem.at[k]) for k, (v, r) in enumerate(zip(rowv, row))]
    for copy in rows:
        copy.start()
    rank_points(pix, ts, em, rt, lhs, carry)
    pack_pixels(em, lhs, psend)
    pown = ship_all(me, 1, psend, pgot, pown_sem, psend_sem, precv_sem)
    build_own(ph, cb, table)
    for copy in rows:
        copy.wait()
    for copy in copies:
        copy.wait()
    build_halo(rx, ry, rc, table)
    radiance(idx, (ox, oy, oz), table, prod, sums, alb, rt, lhs)
    pack(em, lhs, send)
    quarter = me // BLOCK
    own = ship_all(me, 3, send, got, recv_sem.at[quarter], send_sem, recv_sem.at[quarter])
    wait_all(pown, psend, pgot, psend_sem, precv_sem)
    spot_pixels(pgot, spot, frt)
    total[...] = jnp.zeros((96, 128), F32)
    for step in (0, 1, 3, 2):
        b = (quarter + step) & (N // BLOCK - 1)
        quarter_rows = pl.ds(0, 3 * BLOCK)
        pltpu.make_async_copy(send.at[quarter_rows], got.at[quarter_rows], recv_sem.at[b]).wait()
        film_part(b, got, spot, flhs, frt, total)
    film_of(film, total)
    sent = pl.ds(0, 3 * (N - 1))
    pltpu.make_async_copy(send.at[sent], got.at[sent], send_sem).wait()


def per_device(photon_data, block_counts, gather_offsets, gather_blocks, albedo, gather_pixels, tile_slot):
    vmem = pl.BlockSpec(memory_space=pltpu.VMEM)
    dma = pltpu.SemaphoreType.DMA
    return pl.pallas_call(
        kernel,
        out_shape=jax.ShapeDtypeStruct((3, 8, 256), F32),
        in_specs=[vmem, vmem, pl.BlockSpec(memory_space=pl.ANY), vmem, vmem, vmem, vmem],
        out_specs=vmem,
        scratch_shapes=[
            pltpu.VMEM((6, CX, CY, SLOTS), F32),
            pltpu.VMEM((6 * NR, SLOTS), F32),
            pltpu.VMEM((CX * CY, SLOTS), F32),
            pltpu.VMEM((1, G), I32),
            pltpu.VMEM((1, G), F32),
            pltpu.VMEM((1, G), F32),
            pltpu.VMEM((1, G), F32),
            pltpu.SMEM((1, G), I32),
            pltpu.SMEM((1, G), F32),
            pltpu.SMEM((1, G), F32),
            pltpu.SMEM((1, G), F32),
            pltpu.VMEM((3, 16, 32, SLOTS), F32),
            pltpu.VMEM((2, 3, 128, SLOTS), F32),
            pltpu.VMEM((128, G), BF16),
            pltpu.VMEM((RANKS, G), BF16),
            pltpu.VMEM((6 * RANKS, G), BF16),
            pltpu.VMEM((128, 128), F32),
            pltpu.VMEM((2, 6, CY, SLOTS), F32),
            pltpu.VMEM((2, 6, CX, SLOTS), F32),
            pltpu.VMEM((4, 8, SLOTS), F32),
            pltpu.VMEM((2, 6, CY, SLOTS), F32),
            pltpu.VMEM((2, 6, CX, SLOTS), F32),
            pltpu.VMEM((4, 8, SLOTS), F32),
            pltpu.VMEM((N, 1, 128), F32),
            pltpu.VMEM((N, 1, 128), F32),
            pltpu.VMEM((3 * N, 1, 128), F32),
            pltpu.VMEM((3 * N, 1, 128), F32),
            pltpu.VMEM((16, N * 128), BF16),
            pltpu.VMEM((96, N * 128), BF16),
            pltpu.VMEM((128, N * 128), BF16),
            pltpu.VMEM((96, 128), F32),
            dma((3,)), dma((4,)), dma((8,)), dma((8,)), dma, dma((4,)), dma, dma, dma,
        ],
        compiler_params=pltpu.CompilerParams(
            vmem_limit_bytes=67043328, collective_id=1, has_side_effects=True
        ),
        name="photon_film",
    )(
        gather_blocks,
        gather_offsets,
        photon_data,
        block_counts.T,
        albedo,
        gather_pixels.reshape(GROUPS, 128),
        tile_slot.reshape(8, 128),
    )


def solution(mesh):
    in_specs = (
        P(None, "bx", "by", None),
        P("bx", "by"),
        P(None, ("bx", "by")),
        P(None, ("bx", "by")),
        P(None, ("bx", "by")),
        P(("bx", "by")),
        P(),
    )
    out_specs = P(None, ("bx", "by"), None)
    return jax.shard_map(per_device, mesh=mesh, in_specs=in_specs, out_specs=out_specs, check_vma=False)
```

```python
import jax
import jax.numpy as jnp
from jax import lax
from jax.experimental import pallas as pl
from jax.experimental.pallas import tpu as pltpu
from jax.sharding import PartitionSpec as P

MESH = pl.DeviceIdType.MESH
F32, BF16, I32 = jnp.float32, jnp.bfloat16, jnp.int32
NX, NY = 16, 8
N = NX * NY
CX, CY, SLOTS, G = 64, 32, 128, 4096
NXC, NYC = 1024, 256
PITCH = 2 * (CY + 2)
PAD = 8
NR = 4456
RANKS = 96
BLOCK = 32
FAR = 1.0e9
GROUPS = G // 128
FACES = ((1, 0), (-1, 0), (0, 1), (0, -1), (1, 1), (1, -1), (-1, 1), (-1, -1))


def iota(shape, dim):
    return lax.broadcasted_iota(I32, shape, dim)


def hot(mask):
    return mask.astype(F32).astype(BF16)


def split(x):
    high = x.astype(BF16).astype(F32)
    return high, x - high


def across(a, b):
    return lax.dot_general(a, b, (((1,), (1,)), ((), ())), preferred_element_type=F32)


def peer_of(flat):
    return (flat >> 3, flat & 7)


def greet_all(me):
    barrier = pltpu.get_barrier_semaphore()

    def greet(k, unused):
        pl.semaphore_signal(barrier, inc=1, device_id=peer_of((me + k) & (N - 1)), device_id_type=MESH)
        return unused

    lax.fori_loop(1, N, greet, 0)
    return barrier


def prepare(blocks, goff, ix, iy, rowv):
    cells = blocks[...]
    lx = ((cells >> 8) - ix * CX + 1) & (NXC - 1)
    ly = ((cells & (NYC - 1)) - iy * CY + 1) & (NYC - 1)
    x = jnp.minimum(jnp.min(lx, axis=0, keepdims=True), CX)
    y = jnp.minimum(jnp.min(ly, axis=0, keepdims=True), CY)
    rowv[0][...] = PAD + PITCH * x + 2 * y
    rowv[1][...] = 2.0 * (lx[0:1].astype(F32) + goff[0:1, :])
    rowv[2][...] = 2.0 * (ly[0:1].astype(F32) + goff[1:2, :])
    rowv[3][...] = 2.0 * goff[2:3, :]


def spread_counts(cnt, cb):
    counts = cnt[...].astype(F32)
    for x in range(CX):
        cb[x * CY : x * CY + CY, :] = jnp.broadcast_to(counts[:, x : x + 1], (CY, SLOTS))


def change(c, v, x, y):
    if c == 0:
        return 2.0 * (v + x)
    if c == 1:
        return 2.0 * (v + y)
    return 2.0 * v if c == 2 else v


def face_cell(ph, cb, c, row, rows, stride, x, y):
    at = pl.ds(row, rows, stride=stride) if rows > 1 else pl.ds(row, 1)
    v = change(c, ph[c, at, :], x, y)
    slot = iota((rows, SLOTS), 1).astype(F32)
    return jnp.where(slot < cb[at, :], v, FAR) if c == 0 else v


def build_faces_y(ph, cb, fy, fc):
    sub = iota((8, SLOTS), 0).astype(F32)
    for side, (y, to) in enumerate(((CY - 1, 0.0), (0, CY + 1.0))):
        for c in range(6):
            for n in range(CX // 8):
                v = face_cell(ph, cb, c, 8 * n * CY + y, 8, CY, sub + (1.0 + 8 * n), to)
                fy[side, c, 8 * n : 8 * n + 8, :] = v
    for k, (dx, dy) in enumerate(FACES[4:]):
        x, tx = (CX - 1, 0.0) if dx > 0 else (0, CX + 1.0)
        y, ty = (CY - 1, 0.0) if dy > 0 else (0, CY + 1.0)
        for c in range(6):
            fc[k, c : c + 1, :] = face_cell(ph, cb, c, x * CY + y, 1, 1, tx, ty)


def build_faces_x(ph, cb, fx):
    sub = iota((8, SLOTS), 0).astype(F32)
    for side, (x, to) in enumerate(((CX - 1, 0.0), (0, CX + 1.0))):
        for c in range(6):
            for n in range(CY // 8):
                v = face_cell(ph, cb, c, x * CY + 8 * n, 8, 1, to, sub + (1.0 + 8 * n))
                fx[side, c, 8 * n : 8 * n + 8, :] = v


def build_own(ph, cb, table):
    slot = iota((8, SLOTS), 1).astype(F32)
    sub = iota((8, SLOTS), 0).astype(F32)

    def one_x(x, unused):
        xs = (x + 1).astype(F32)
        for n in range(CY // 8):
            at = pl.ds(pl.multiple_of(x * CY + 8 * n, 8), 8)
            live = slot < cb[at, :]
            for c in range(6):
                v = change(c, ph[c, at, :], xs, sub + (1.0 + 8 * n))
                if c == 0:
                    v = jnp.where(live, v, FAR)
                base = c * NR + PAD + (x + 1) * PITCH + 2 * (1 + 8 * n)
                table[pl.ds(base, 8, stride=2), :] = v
                table[pl.ds(base - PITCH + 1, 8, stride=2), :] = v
        return unused

    lax.fori_loop(0, CX, one_x, 0)


def build_halo(rx, ry, rc, table):
    for c in range(6):
        for side, base in enumerate((c * NR + PAD, c * NR + PAD + CX * PITCH + 1)):
            for n in range(CY // 8):
                table[pl.ds(base + 2 + 16 * n, 8, stride=2), :] = rx[side, c, 8 * n : 8 * n + 8, :]
        for side, y in enumerate((0, CY + 1)):
            for n in range(CX // 8):
                v = ry[side, c, 8 * n : 8 * n + 8, :]
                base = c * NR + PAD + (8 * n + 1) * PITCH + 2 * y
                table[pl.ds(base, 8, stride=PITCH), :] = v
                table[pl.ds(base - PITCH + 1, 8, stride=PITCH), :] = v
        for k, (dx, dy) in enumerate(FACES[4:]):
            y = 0 if dy > 0 else CY + 1
            base = c * NR + PAD + (0 if dx > 0 else CX * PITCH + 1) + 2 * y
            table[pl.ds(base, 1), :] = rc[k, c : c + 1, :]


def rank_points(pix, ts, em, rt, lhs, carry):
    t = ts[...]
    lookup = jnp.concatenate([t >> 3, t & 7], axis=0).astype(F32).astype(BF16)
    rows, cols = iota((128, 128), 0), iota((128, 128), 1)
    before = jnp.concatenate([hot(rows < cols), jnp.ones((128, 128), BF16)], axis=1)
    eight = iota((8, 128), 0)
    carry[...] = jnp.zeros((128, 128), F32)

    def tiles(i, unused):
        for u in range(4):
            j = 4 * i + u
            at = pl.ds(pl.multiple_of(j * 128, 128), 128)
            pixel = pix[pl.ds(j, 1), :]
            image = pixel >> 8
            found = jnp.dot(lookup, hot(rows == (image & 127)), preferred_element_type=F32)
            pick = eight == (image >> 7)
            owner = jnp.sum(jnp.where(pick, found[:8], 0.0), axis=0, keepdims=True)
            inner = jnp.sum(jnp.where(pick, found[8:], 0.0), axis=0, keepdims=True)
            mine = rows == owner.astype(I32)
            chosen = hot(mine)
            em[:, at] = chosen
            counts = jnp.dot(chosen, before, preferred_element_type=F32)
            rank = jnp.sum(jnp.where(mine, counts[:, :128] + carry[...], 0.0), axis=0, keepdims=True)
            carry[...] += counts[:, 128:]
            place = hot(rows == rank.astype(I32))[:RANKS]
            rt[:, at] = place
            local = inner * 256.0 + (pixel & 255).astype(F32)
            high = jnp.floor(local * (1.0 / 128.0))
            lhs[0:RANKS, at] = place * high.astype(BF16)
            lhs[RANKS : 2 * RANKS, at] = place * (local - 128.0 * high).astype(BF16)
        return unused

    lax.fori_loop(0, GROUPS // 4, tiles, 0)


def by_owner(part):
    whole = jnp.concatenate([part, jnp.zeros((128 - RANKS, 128), F32)], axis=0)
    return whole.T


def pack_pixels(em, lhs, psend):
    part = across(lhs[0 : 2 * RANKS, :], em[...])
    psend.reshape(N, 128)[...] = by_owner(128.0 * part[:RANKS] + part[RANKS:])


def weigh_tile(j, idx, off, table, prod, sums, between):
    half = iota((8, SLOTS), 0) < 4
    for u in range(16):
        if u in (2, 6, 10):
            between(u // 4)
        g0 = j * 128 + 8 * u
        for pair in range(4):
            p, q = g0 + 2 * pair, g0 + 2 * pair + 1
            rp, rq = idx[0, p], idx[0, q] - 4
            v = []
            for c in range(6):
                a = table[pl.ds(rp + c * NR, 8), :]
                b = table[pl.ds(rq + c * NR, 8), :]
                if c < 3:
                    a, b = a - off[c][0, p], b - off[c][0, q]
                v.append(jnp.where(half, a, b))
            w = jnp.maximum(1.0 - (v[0] * v[0] + v[1] * v[1] + v[2] * v[2]), 0.0)
            for c in range(3):
                prod[c, u, 8 * pair : 8 * pair + 8, :] = w * v[3 + c]
        for c in range(3):
            s = [prod[c, u, pl.ds(k, 8, stride=4), :] for k in range(4)]
            sums[c, 8 * u : 8 * u + 8, :] = (s[0] + s[1]) + (s[2] + s[3])


def place_tile(j, alb, sums, rt, lhs, channels=(0, 1, 2)):
    at = pl.ds(pl.multiple_of(j * 128, 128), 128)
    ones = jnp.ones((8, 256), BF16)
    place = rt[:, at]
    for c in channels:
        whole = sums[c]
        high = whole.astype(BF16)
        low = (whole - high.astype(F32)).astype(BF16)
        total = across(ones, jnp.concatenate([high, low], axis=1))
        for k, row in enumerate(split(total[0:1] * alb[c : c + 1, at])):
            first = RANKS * (2 * c + k)
            lhs[first : first + RANKS, at] = place * row.astype(BF16)


def radiance(idx, off, table, prod, sums, alb, rt, lhs):
    def tiles(i, unused):
        for k in range(4):
            j = 4 * i + k

            def between(c):
                place_tile(jnp.maximum(j - 1, 0), alb, sums.at[1 - k % 2], rt, lhs, (c,))

            weigh_tile(j, idx, off, table, prod, sums.at[k % 2], between)
        return unused

    sums[...] = jnp.zeros((2, 3, 128, SLOTS), F32)
    lax.fori_loop(0, GROUPS // 4, tiles, 0)
    place_tile(GROUPS - 1, alb, sums.at[1], rt, lhs)


def pack(em, lhs, send):
    part = across(lhs[...], em[...])
    flat = send.reshape(3 * N, 128)
    for c in range(3):
        a = part[2 * c * RANKS : (2 * c + 1) * RANKS]
        b = part[(2 * c + 1) * RANKS : (2 * c + 2) * RANKS]
        flat[pl.ds(c, 128, stride=3), :] = by_owner(a + b)


def spot_pixels(pgot, spot, rt):
    rows = iota((128, 128), 0)
    sixteen = iota((16, 128), 0)

    def sources(i, unused):
        for u in range(4):
            s = 4 * i + u
            at = pl.ds(pl.multiple_of(s * 128, 128), 128)
            pixel = pgot[s].astype(I32)
            rt[:, at] = hot(rows == (pixel & 127))
            spot[:, at] = hot(sixteen == ((pixel >> 7) & 1) * 8 + (pixel >> 8))
        return unused

    lax.fori_loop(0, N // 4, sources, 0)


def film_part(b, got, spot, lhs, rt, total):
    def sources(i, unused):
        for u in range(4):
            s = 4 * i + u
            at = pl.ds(pl.multiple_of(s * 128, 128), 128)
            where = spot[:, at]
            for c in range(3):
                for k, part in enumerate(split(got[3 * s + c])):
                    first = 16 * (2 * c + k)
                    lhs[first : first + 16, at] = where * part.astype(BF16)
        return unused

    lax.fori_loop(b * (BLOCK // 4), (b + 1) * (BLOCK // 4), sources, 0)
    at = pl.ds(pl.multiple_of(b * (BLOCK * 128), 128), BLOCK * 128)
    total[...] += across(lhs[:, at], rt[:, at])


def film_of(film, total):
    for c in range(3):
        both = total[32 * c : 32 * c + 16, :] + total[32 * c + 16 : 32 * c + 32, :]
        film[c, :, 0:128] = both[:8]
        film[c, :, 128:256] = both[8:]


def ship_all(me, rows, send, got, own_sem, send_sem, recv_sem):
    here = pl.ds(me * rows, rows)
    own = pltpu.make_async_copy(send.at[here], got.at[here], own_sem)
    own.start()

    def ship(k, unused):
        peer = (me + k) & (N - 1)
        pltpu.make_async_remote_copy(
            src_ref=send.at[pl.ds(peer * rows, rows)],
            dst_ref=got.at[here],
            send_sem=send_sem,
            recv_sem=recv_sem,
            device_id=peer_of(peer),
            device_id_type=MESH,
        ).start()
        return unused

    for first in (64, 32, 96, 0):
        lax.fori_loop(max(first, 1), first + 32, ship, 0)
    return own


def wait_all(own, send, got, send_sem, recv_sem):
    own.wait()
    for sem in (recv_sem, send_sem):
        pltpu.make_async_copy(send.at[pl.ds(0, N - 1)], got.at[pl.ds(0, N - 1)], sem).wait()


def kernel(
    blocks, goff, photons, cnt, alb, pix, ts, film,
    ph4, table, cb, idxv, oxv, oyv, ozv, idx, ox, oy, oz, prod, sums, em, rt, lhs, carry,
    fx, fy, fc, rx, ry, rc, psend, pgot, send, got, spot, flhs, frt, total,
    ph_sem, idx_sem, face_send, face_recv, send_sem, recv_sem, pown_sem, psend_sem, precv_sem,
):
    ix, iy = lax.axis_index("bx"), lax.axis_index("by")
    me = ix * NY + iy
    loads = []
    for k, (first, last) in enumerate(((0, 8), (CY - 8, CY), (8, CY - 8))):
        part = (slice(None), slice(None), pl.ds(first, last - first))
        loads.append(pltpu.make_async_copy(photons.at[part], ph4.at[part], ph_sem.at[k]))
        loads[k].start()
    ph = ph4.reshape(6, CX * CY, SLOTS)
    barrier = greet_all(me)
    spread_counts(cnt, cb)
    loads[0].wait()
    loads[1].wait()
    build_faces_y(ph, cb, fy, fc)
    pl.semaphore_wait(barrier, N - 1)
    copies = []
    for k, (dx, dy) in enumerate(FACES):
        source, target = ((fx, rx), (fy, ry), (fc, rc))[min(k // 2, 2)]
        k2 = k % 2 if k < 4 else k - 4
        copy = pltpu.make_async_remote_copy(
            src_ref=source.at[k2],
            dst_ref=target.at[k2],
            send_sem=face_send.at[k],
            recv_sem=face_recv.at[k],
            device_id=((ix + dx) & (NX - 1), (iy + dy) & (NY - 1)),
            device_id_type=MESH,
        )
        copies.append(copy)
    for k in (2, 3, 4, 5, 6, 7):
        copies[k].start()
    loads[2].wait()
    build_faces_x(ph, cb, fx)
    for k in (0, 1):
        copies[k].start()
    rowv, row = (idxv, oxv, oyv, ozv), (idx, ox, oy, oz)
    prepare(blocks, goff, ix, iy, rowv)
    rows = [pltpu.make_async_copy(v, r, idx_sem.at[k]) for k, (v, r) in enumerate(zip(rowv, row))]
    for copy in rows:
        copy.start()
    rank_points(pix, ts, em, rt, lhs, carry)
    pack_pixels(em, lhs, psend)
    pown = ship_all(me, 1, psend, pgot, pown_sem, psend_sem, precv_sem)
    build_own(ph, cb, table)
    for copy in rows:
        copy.wait()
    for copy in copies:
        copy.wait()
    build_halo(rx, ry, rc, table)
    radiance(idx, (ox, oy, oz), table, prod, sums, alb, rt, lhs)
    pack(em, lhs, send)
    quarter = me // BLOCK
    own = ship_all(me, 3, send, got, recv_sem.at[quarter], send_sem, recv_sem.at[quarter])
    wait_all(pown, psend, pgot, psend_sem, precv_sem)
    spot_pixels(pgot, spot, frt)
    total[...] = jnp.zeros((96, 128), F32)
    for step in (0, 1, 3, 2):
        b = (quarter + step) & (N // BLOCK - 1)
        quarter_rows = pl.ds(0, 3 * BLOCK)
        pltpu.make_async_copy(send.at[quarter_rows], got.at[quarter_rows], recv_sem.at[b]).wait()
        film_part(b, got, spot, flhs, frt, total)
    film_of(film, total)
    sent = pl.ds(0, 3 * (N - 1))
    pltpu.make_async_copy(send.at[sent], got.at[sent], send_sem).wait()


def per_device(photon_data, block_counts, gather_offsets, gather_blocks, albedo, gather_pixels, tile_slot):
    vmem = pl.BlockSpec(memory_space=pltpu.VMEM)
    dma = pltpu.SemaphoreType.DMA
    return pl.pallas_call(
        kernel,
        out_shape=jax.ShapeDtypeStruct((3, 8, 256), F32),
        in_specs=[vmem, vmem, pl.BlockSpec(memory_space=pl.ANY), vmem, vmem, vmem, vmem],
        out_specs=vmem,
        scratch_shapes=[
            pltpu.VMEM((6, CX, CY, SLOTS), F32),
            pltpu.VMEM((6 * NR, SLOTS), F32),
            pltpu.VMEM((CX * CY, SLOTS), F32),
            pltpu.VMEM((1, G), I32),
            pltpu.VMEM((1, G), F32),
            pltpu.VMEM((1, G), F32),
            pltpu.VMEM((1, G), F32),
            pltpu.SMEM((1, G), I32),
            pltpu.SMEM((1, G), F32),
            pltpu.SMEM((1, G), F32),
            pltpu.SMEM((1, G), F32),
            pltpu.VMEM((3, 16, 32, SLOTS), F32),
            pltpu.VMEM((2, 3, 128, SLOTS), F32),
            pltpu.VMEM((128, G), BF16),
            pltpu.VMEM((RANKS, G), BF16),
            pltpu.VMEM((6 * RANKS, G), BF16),
            pltpu.VMEM((128, 128), F32),
            pltpu.VMEM((2, 6, CY, SLOTS), F32),
            pltpu.VMEM((2, 6, CX, SLOTS), F32),
            pltpu.VMEM((4, 8, SLOTS), F32),
            pltpu.VMEM((2, 6, CY, SLOTS), F32),
            pltpu.VMEM((2, 6, CX, SLOTS), F32),
            pltpu.VMEM((4, 8, SLOTS), F32),
            pltpu.VMEM((N, 1, 128), F32),
            pltpu.VMEM((N, 1, 128), F32),
            pltpu.VMEM((3 * N, 1, 128), F32),
            pltpu.VMEM((3 * N, 1, 128), F32),
            pltpu.VMEM((16, N * 128), BF16),
            pltpu.VMEM((96, N * 128), BF16),
            pltpu.VMEM((128, N * 128), BF16),
            pltpu.VMEM((96, 128), F32),
            dma((3,)), dma((4,)), dma((8,)), dma((8,)), dma, dma((4,)), dma, dma, dma,
        ],
        compiler_params=pltpu.CompilerParams(
            vmem_limit_bytes=67043328, collective_id=1, has_side_effects=True
        ),
        name="photon_film",
    )(
        gather_blocks,
        gather_offsets,
        photon_data,
        block_counts.T,
        albedo,
        gather_pixels.reshape(GROUPS, 128),
        tile_slot.reshape(8, 128),
    )


def solution(mesh):
    in_specs = (
        P(None, "bx", "by", None),
        P("bx", "by"),
        P(None, ("bx", "by")),
        P(None, ("bx", "by")),
        P(None, ("bx", "by")),
        P(("bx", "by")),
        P(),
    )
    out_specs = P(None, ("bx", "by"), None)
    return jax.shard_map(per_device, mesh=mesh, in_specs=in_specs, out_specs=out_specs, check_vma=False)
```
